256 devices in a mesh: member: 2 (over y), lat: 128 (over z, x, core).
Axes of the slice: x: 4, y: 2, z: 16, core: 2. Of those that a mesh axis runs over, the one named last changes fastest.
The devices are a block of a 4x16x16 slice.
Arguments:
- increment: float32 [274, 2048, 128], P('member', 'lat'), parts along dimension 0, may hold values from -6 to 6
- filter_taps: int32 [4, 2, 2, 5], replicated, may hold values from 1 to 8
- band_roots: float32 [5, 137, 137], replicated, may hold values from -1 to 1
Outputs:
- adjoint: float32 [274, 2048, 128], P('member', 'lat'), parts along dimension 0
The draws below stay inside these ranges and needn't reach their ends.
There are 2 independent parts, one for each index of `member`. The reference program is written for one: setup_inputs(seed, part) draws one part's arguments, and reference() takes and returns one part's arrays. A program takes and returns all parts, laid end to end along the dimension named above; an argument that names none is the same for every part. Nothing has to cross between parts.
All inputs are finite; a program needn't handle non-finite values.
Results may differ from the reference program's by a relative error of at most 0.0001.
Values sent between devices are 32-bit elements; how exact they have to be, the bound alone decides.
No kernel may reach another device: no remote copies, remote signals or barrier semaphores. Data moves between devices by JAX's collectives and lax.ppermute only.
A program may use at most 64 MiB of HBM per device.

```python
import math
import jax
import jax.numpy as jnp
from jax import lax

LEV = 137
NLON = 128
LEVELS = 4
BANDS = 5
NLAT = 2048


def with_ends(values, rng, least, top_value):
    index_at = [jax.random.randint(jax.random.fold_in(rng, axis), (), 0, length) for axis, length in enumerate(values.shape)]
    main_axis = values.shape.index(max(values.shape))
    next_to = index_at[:main_axis] + [(index_at[main_axis] + 1) % values.shape[main_axis]] + index_at[main_axis + 1:]
    return values.at[tuple(index_at)].set(least).at[tuple(next_to)].set(top_value)


def levels(key, extent, split, least, high):
    gain = 1.0
    for dim, blocks in split:
        heights = jax.random.uniform(jax.random.fold_in(jax.random.fold_in(key, 6), dim), (blocks,), jnp.float32, least / len(split), high / len(split))
        gain = gain * jnp.repeat(jnp.exp(heights), extent[dim] // blocks).reshape((-1,) + (1,) * (len(extent) - 1 - dim))
    return gain


def normal_values(key, extent, scale, reach, pieces=(), held_as=jnp.bfloat16):
    values = scale * jax.random.normal(key, extent, jnp.float32)
    if pieces:
        values = values * levels(key, extent, pieces, -0.22, 0.18)
    return jnp.clip(values, -reach, reach).astype(held_as)


def setup_inputs(seed: int = 0, part: int = 0) -> dict:
    arg_keys = jax.random.split(jax.random.key(seed), 4)
    part_keys = jax.random.split(jax.random.fold_in(arg_keys[3], part), 4)
    increment = normal_values(part_keys[0], (LEV, NLAT, NLON), 1.0, 6.0, ((1, 128),), jnp.float32)
    filter_taps = with_ends(jax.random.randint(arg_keys[1], (LEVELS, 2, 2, 5), 1, 9), jax.random.fold_in(arg_keys[1], 1), 1, 8).astype(jnp.int32)
    band_roots = normal_values(arg_keys[2], (BANDS, LEV, LEV), 0.17, 1.0, (), jnp.float32)
    return {"increment": increment, "filter_taps": filter_taps, "band_roots": band_roots}


ROOT_TWO = math.sqrt(2.0)

def make_filters(filter_taps):
    coeffs = filter_taps.astype(jnp.float32)
    sign_pattern = jnp.array([1.0, -1.0, 1.0, -1.0, 1.0], dtype=jnp.float32)
    lowpass = ROOT_TWO * coeffs[:, :, 0] / lax.optimization_barrier(jnp.sum(coeffs[:, :, 0], axis=-1, keepdims=True))
    highpass = sign_pattern * coeffs[:, :, 1] / jnp.sqrt(lax.optimization_barrier(jnp.sum(coeffs[:, :, 1] * coeffs[:, :, 1], axis=-1, keepdims=True)))
    return jnp.stack([lowpass, highpass], axis=2)

def filter_down(padded, coeffs, length, along):
    summed = coeffs[0] * lax.slice_in_dim(padded, 0, length, 2, along)
    for offset in range(1, 5):
        summed = summed + coeffs[offset] * lax.slice_in_dim(padded, offset, offset + length, 2, along)
    return summed

def filter_up(padded, coeffs, length, along):
    summed = coeffs[0] * lax.slice_in_dim(padded, 4, 4 + length, 1, along)
    for offset in range(1, 5):
        summed = summed + coeffs[offset] * lax.slice_in_dim(padded, 4 - offset, 4 - offset + length, 1, along)
    return summed

def spread_zeros(values, along):
    stacked = jnp.stack([values, jnp.zeros_like(values)], axis=along + 1)
    new_shape = values.shape[:along] + (2 * values.shape[along],) + values.shape[along + 1:]
    return stacked.reshape(new_shape)

def pad_cols(values):
    padding = [(0, 0)] * (values.ndim - 1) + [(2, 2)]
    return jnp.pad(values, padding)

def analyze(values, level_filters, row_rim):
    row_count = values.shape[1]
    col_count = values.shape[2]
    padded = row_rim(values[None], 2)[0]
    halves = jnp.stack([filter_down(padded, level_filters[0, 0], row_count, 1), filter_down(padded, level_filters[0, 1], row_count, 1)])
    widened = pad_cols(halves)
    low_parts = filter_down(widened, level_filters[1, 0], col_count, 3)
    high_parts = filter_down(widened, level_filters[1, 1], col_count, 3)
    return (low_parts[0], jnp.stack([high_parts[0], low_parts[1], high_parts[1]]))

def synthesize(coarse, details, level_filters, row_rim):
    row_count = 2 * coarse.shape[1]
    col_count = 2 * coarse.shape[2]
    low_parts = pad_cols(spread_zeros(jnp.stack([coarse, details[1]]), 3))
    high_parts = pad_cols(spread_zeros(jnp.stack([details[0], details[2]]), 3))
    halves = filter_up(low_parts, level_filters[1, 0], col_count, 3) + filter_up(high_parts, level_filters[1, 1], col_count, 3)
    padded = spread_zeros(row_rim(halves, 1), 2)
    return filter_up(padded[0], level_filters[0, 0], row_count, 1) + filter_up(padded[1], level_filters[0, 1], row_count, 1)

def vertical(matrix, band, transposed):
    chosen = matrix.T if transposed else matrix
    return jnp.einsum('ij,...jrc->...irc', chosen, band, precision=lax.Precision.HIGHEST, preferred_element_type=jnp.float32)

def zero_rim(values, rim_width):
    padding = [(0, 0)] * values.ndim
    padding[2] = (rim_width, rim_width)
    return jnp.pad(values, padding)

def transform(values, level_filters, band_roots, transposed):
    band_list = []
    coarse = values
    for level_index in range(LEVELS):
        coarse, details = analyze(coarse, level_filters[level_index], zero_rim)
        band_list.append(vertical(band_roots[level_index], details, transposed))
    coarse = vertical(band_roots[LEVELS], coarse, transposed)
    for level_index in reversed(range(LEVELS)):
        coarse = synthesize(coarse, band_list[level_index], level_filters[level_index], zero_rim)
    return coarse

def reference(increment, filter_taps, band_roots):
    level_filters = make_filters(filter_taps)
    shaped = transform(increment, level_filters, band_roots, False)
    return transform(shaped, level_filters, band_roots, True)
```

```python
import functools
import math

import jax
import jax.numpy as jnp
from jax import lax
from jax.experimental import pallas as pl
from jax.experimental.pallas import tpu as pltpu
from jax.sharding import PartitionSpec as P

LEVELS = 4
TAPS = 5
ROOT_TWO = math.sqrt(2.0)
F32 = jnp.float32
BF16 = jnp.bfloat16
MIB = 1024 * 1024

ROWS = 16
OWN = (8, 4, 2, 1)
FIRST = -1
LAST = (8, 5, 3, 2)
COUNT = (10, 7, 5, 4)
BASE = (0, 10, 17, 22)
SLOTS = 26
LANES = 128
PAD = 144
KPAD = 256


def dot(a, b):
    return lax.dot_general(a, b, (((1,), (0,)), ((), ())), preferred_element_type=F32)


def dot_t(a, b):
    return lax.dot_general(a, b, (((1,), (1,)), ((), ())), preferred_element_type=F32)


def split(values):
    high = values.astype(BF16)
    return high, (values - high.astype(F32)).astype(BF16)


def slot(level, index):
    return BASE[level] + index - FIRST


def lane_ids(rows):
    return lax.broadcasted_iota(jnp.int32, (rows, LANES), 1)


def write_filters(taps_ref, filt_ref):
    signs = (1.0, -1.0, 1.0, -1.0, 1.0)
    ones = jnp.full((1, LANES), 1.0, F32)
    for level in range(LEVELS):
        for way in range(2):
            low = [taps_ref[level, way, 0, k].astype(F32) * ones for k in range(TAPS)]
            high = [taps_ref[level, way, 1, k].astype(F32) * ones for k in range(TAPS)]
            low_scale = ROOT_TWO / functools.reduce(jnp.add, low)
            high_scale = 1.0 / jnp.sqrt(functools.reduce(jnp.add, [h * h for h in high]))
            row = (level * 2 + way) * 2 * TAPS
            for k in range(TAPS):
                filt_ref[row + k : row + k + 1, :] = low[k] * low_scale
                filt_ref[row + TAPS + k : row + TAPS + k + 1, :] = (signs[k] * high[k]) * high_scale


def coeffs(filt_ref, level, way, kind):
    row = ((level * 2 + way) * 2 + kind) * TAPS
    return [filt_ref[row + k : row + k + 1, :] for k in range(TAPS)]


def write_weights(filt_ref, w0_ref, w_ref, ww_ref):
    row = lax.broadcasted_iota(jnp.int32, (LANES, LANES), 0)
    lane = lax.broadcasted_iota(jnp.int32, (LANES, LANES), 1)
    composed = None
    for level in range(LEVELS):
        half = (LANES // 2) >> level
        low = coeffs(filt_ref, level, 1, 0)
        high = coeffs(filt_ref, level, 1, 1)
        is_low = lane < half
        tap = row - 2 * jnp.where(is_low, lane, lane - half) + 2
        inside = (lane < 2 * half) & (row < 2 * half)
        step = jnp.zeros((LANES, LANES), F32)
        for k in range(TAPS):
            chosen = jnp.where(is_low, low[k], high[k])
            step = jnp.where(inside & (tap == k), chosen, step)
        if composed is None:
            composed = step
        else:
            composed = lax.dot_general(
                composed, step, (((1,), (0,)), ((), ())),
                precision=lax.Precision.HIGHEST, preferred_element_type=F32,
            )
        zeros = jnp.zeros((LANES, LANES), BF16)
        if level == 0:
            d_high, d_low = split(composed)
            moved = jnp.where(lane < half, pltpu.roll(composed, LANES - half, 1), 0.0)
            a_high, a_low = split(moved)
            w0_ref[0:LANES, 0:128] = zeros
            w0_ref[0:LANES, 128:256] = a_high
            w0_ref[0:LANES, 256:384] = zeros
            w0_ref[0:LANES, 384:512] = a_low
            w0_ref[LANES:256, 0:128] = d_high
            w0_ref[LANES:256, 128:256] = zeros
            w0_ref[LANES:256, 256:384] = d_low
            w0_ref[LANES:256, 384:512] = zeros
        else:
            moved = jnp.where((lane >= 2 * half) & (lane < 3 * half), pltpu.roll(composed, half, 1), 0.0)
            if level == LEVELS - 1:
                moved = moved + jnp.where(
                    (lane >= 3 * half) & (lane < 4 * half), pltpu.roll(composed, 3 * half, 1), 0.0
                )
            for part, values in ((0, moved), (1, composed)):
                rows = slice(part * LANES, part * LANES + LANES)
                v_high, v_low = split(values)
                w_ref[level - 1, rows, 0:128] = v_high
                w_ref[level - 1, rows, 128:256] = v_low
                ww_ref[level - 1, rows, 0:128] = v_high
                ww_ref[level - 1, rows, 128:256] = v_high


def edge_flags():
    place = lax.axis_index("lat")
    count = lax.axis_size("lat")
    lower = jnp.where(place == 0, 0.0, 1.0).astype(F32)
    upper = jnp.where(place == count - 1, 0.0, 1.0).astype(F32)
    return lower, upper


def masked(values, index, own, flags):
    if index < 0:
        return values * flags[0]
    if index >= own:
        return values * flags[1]
    return values


def latitude_analysis(rows, filt_ref, flags):
    out = {}
    for level in range(LEVELS):
        low = coeffs(filt_ref, level, 0, 0)
        high = coeffs(filt_ref, level, 0, 1)
        smooth = {}
        for index in range(FIRST, LAST[level] + 1):
            a = d = None
            for k in range(TAPS):
                source = rows.get(2 * index - 2 + k)
                if source is None:
                    continue
                a = low[k] * source if a is None else a + low[k] * source
                d = high[k] * source if d is None else d + high[k] * source
            if level < LEVELS - 1:
                a = masked(a, index, OWN[level], flags)
            smooth[index] = a
            out[slot(level, index)] = (a, d)
        rows = smooth
    return out


def latitude_synthesis(pick, filt_ref, flags):
    rows = None
    for level in reversed(range(LEVELS)):
        low = coeffs(filt_ref, level, 0, 0)
        high = coeffs(filt_ref, level, 0, 1)
        first, last = (FIRST, LAST[level - 1]) if level else (0, ROWS - 1)
        smooth, sharp = {}, {}
        for index in range(FIRST, LAST[level] + 1):
            a, d = pick(slot(level, index))
            smooth[index] = a if rows is None else a + rows[index]
            sharp[index] = d
        out = {}
        for r in range(first, last + 1):
            total = None
            for index in range(FIRST, LAST[level] + 1):
                k = r - 2 * index + 2
                if 0 <= k < TAPS:
                    term = low[k] * smooth[index] + high[k] * sharp[index]
                    total = term if total is None else total + term
            out[r] = masked(total, r, OWN[level - 1], flags) if level else total
        rows = out
    return rows


def pack(c0, c1, c2, c3, c1b=None, c2b=None):
    lane = lane_ids(PAD)
    extra = jnp.zeros((PAD, LANES), F32) if c2b is None else pltpu.roll(c2b, 80, 1)
    tiles = [
        c0[:, 0:128],
        jnp.where(lane < 64, c0[:, 128:256], jnp.where(lane < 112, pltpu.roll(c2, 64, 1), extra)),
        jnp.where(lane < 96, c1, pltpu.roll(c3, 96, 1)),
    ]
    if c1b is not None:
        tiles.append(jnp.where(lane < 96, c1b, pltpu.roll(c2b, 96, 1)))
    return tiles


def unpack(ref):
    tile1 = ref[:, 128:256]
    tile2 = ref[:, 256:384]
    parts = [ref[:, 0:256], tile2, pltpu.roll(tile1, 64, 1), pltpu.roll(tile2, 32, 1)]
    if ref.shape[1] > 384:
        tile3 = ref[:, 384:512]
        lane = lane_ids(PAD)
        parts += [tile3, jnp.where(lane < 32, pltpu.roll(tile3, 32, 1), pltpu.roll(tile1, 48, 1))]
    return parts


def pack_coarse(c3):
    lane = lane_ids(40)
    last = jnp.concatenate([c3[120:144], jnp.zeros((16, LANES), F32)], axis=0)
    return jnp.where(
        lane < 32,
        c3[0:40],
        jnp.where(
            lane < 64,
            pltpu.roll(c3[40:80], 32, 1),
            jnp.where(lane < 96, pltpu.roll(c3[80:120], 64, 1), pltpu.roll(last, 96, 1)),
        ),
    )


def unpack_coarse(ref):
    values = ref[...]
    parts = [values] + [pltpu.roll(values, LANES - 32 * q, 1) for q in (1, 2, 3)]
    return jnp.concatenate(parts[:3] + [parts[3][0:24]], axis=0)


def store_split(hi_ref, lo_ref, out, at):
    for place, (a, d) in out.items():
        for part, values in ((0, a), (1, d)):
            lanes = slice(part * LANES, part * LANES + LANES)
            high, low = split(values)
            hi_ref[place, at, lanes] = high
            lo_ref[place, at, lanes] = low


def longitude_analysis(hi_ref, lo_ref, w0_ref, w_ref, c0_ref, c1_ref, c2_ref, c3_ref, up_ref, down_ref, far_ref):
    def level0(index):
        s = slot(0, index)
        w_high, w_low = w0_ref[:, 0:256], w0_ref[:, 256:512]
        high = hi_ref[s]
        return dot(high, w_high) + dot(high, w_low) + dot(lo_ref[s], w_high)

    def others(level, index):
        s = slot(level, index)
        both = dot(hi_ref[s], w_ref[level - 1])
        return both[:, 0:128] + both[:, 128:256] + dot(lo_ref[s], w_ref[level - 1, :, 0:128])

    c3 = {i: others(3, i) for i in range(-1, 3)}
    far_ref[...] = pack_coarse(c3[2])
    up = pack(level0(8), others(1, 4), others(2, 2), c3[1], others(1, 5), others(2, 3))
    for t, tile in enumerate(up):
        up_ref[:, t * LANES : t * LANES + LANES] = tile
    down = pack(level0(-1), others(1, -1), others(2, -1), c3[-1])
    for t, tile in enumerate(down):
        down_ref[:, t * LANES : t * LANES + LANES] = tile
    c3_ref[...] = c3[0]
    for i in range(8):
        c0_ref[i] = level0(i)
    for i in range(4):
        c1_ref[i // 2, :, (i % 2) * 128 : (i % 2) * 128 + 128] = others(1, i)
    for i in range(2):
        c2_ref[:, i * 128 : i * 128 + 128] = others(2, i)


def longitude_synthesis(
    y0_ref, y1_ref, y2_ref, y3_ref, below_ref, above_ref, far_ref, w0_ref, w_ref, ww_ref, u_ref
):
    below = unpack(below_ref)
    above = unpack(above_ref)
    far = unpack_coarse(far_ref)
    c0 = {-1: below[0], 8: above[0]}
    c1 = {-1: below[1], 4: above[1], 5: above[4]}
    c2 = {-1: below[2], 2: above[2], 3: above[5]}
    c3 = {-1: below[3], 1: above[3], 2: far, 0: y3_ref[...]}
    for i in range(8):
        c0[i] = y0_ref[i]
    for i in range(4):
        c1[i] = y1_ref[i // 2, :, (i % 2) * 128 : (i % 2) * 128 + 128]
    for i in range(2):
        c2[i] = y2_ref[:, i * 128 : i * 128 + 128]
    for i, values in c0.items():
        high, low = split(values)
        w_high, w_low = w0_ref[:, 0:256], w0_ref[:, 256:512]
        u_ref[slot(0, i)] = dot_t(high, w_high) + dot_t(low, w_high) + dot_t(high, w_low)
    for level, group in ((1, c1), (2, c2), (3, c3)):
        for i, values in group.items():
            high, low = split(values)
            pair = jnp.concatenate([high, low], axis=1)
            u_ref[slot(level, i)] = dot_t(pair, ww_ref[level - 1]) + dot_t(high, w_ref[level - 1, :, 128:256])


def pick_at(u_ref, at):
    def pick(place):
        return u_ref[place, at, 0:128], u_ref[place, at, 128:256]

    return pick


def first_kernel(taps_ref, x_ref, *rest):
    filt_ref, w0_ref, w_ref, ww_ref, *outs = rest[:-2]
    hi_ref, lo_ref = rest[-2:]
    write_filters(taps_ref, filt_ref)
    flags = edge_flags()
    write_weights(filt_ref, w0_ref, w_ref, ww_ref)

    def chunk(c, carry):
        start = pl.multiple_of(c * (16 * ROWS), 16 * ROWS)
        rows = {r: x_ref[pl.ds(start + r, 16, stride=ROWS), :] for r in range(ROWS)}
        at = pl.ds(pl.multiple_of(c * 16, 16), 16)
        store_split(hi_ref, lo_ref, latitude_analysis(rows, filt_ref, flags), at)
        return carry

    lax.fori_loop(0, 8, chunk, 0)
    top = lax.broadcasted_iota(jnp.int32, (8, LANES), 0) == 0
    rows = {}
    for r in range(ROWS):
        head = x_ref[pl.ds(128 * ROWS + r, 8, stride=ROWS), :]
        tail = jnp.where(top, x_ref[136 * ROWS + r : 136 * ROWS + r + 1, :], 0.0)
        rows[r] = jnp.concatenate([head, tail], axis=0)
    store_split(hi_ref, lo_ref, latitude_analysis(rows, filt_ref, flags), slice(128, 144))
    longitude_analysis(hi_ref, lo_ref, w0_ref, w_ref, *outs)


def vertical_kernel(m_ref, c0_ref, c1_ref, c2_ref, c3_ref, below_ref, above_ref, far_ref, y0_ref, y1_ref, y2_ref, y3_ref,
                    up_ref, down_ref, far_out_ref):
    below = unpack(below_ref)
    above = unpack(above_ref)
    far = unpack_coarse(far_ref)

    def apply(band, values):
        high, low = split(values)
        zeros = jnp.zeros((KPAD - PAD, values.shape[1]), BF16)
        high = jnp.concatenate([high, zeros], axis=0)
        low = jnp.concatenate([low, zeros], axis=0)
        both = dot(m_ref[band], high)
        return both[0:PAD] + both[PAD:] + dot(m_ref[band, 0:PAD], low)

    c3 = c3_ref[...] + below[3] + above[3] + far
    lane = lane_ids(PAD)
    y3 = jnp.where(lane < 24, apply(3, c3), apply(4, c3))
    y3_ref[...] = y3
    far_out_ref[...] = pack_coarse(y3)
    c2 = c2_ref[...]
    y2 = apply(2, jnp.concatenate([c2[:, 0:128] + below[2], c2[:, 128:256] + below[5] + above[2]], axis=1))
    y2_ref[...] = y2
    c1 = c1_ref[0]
    y1_low = apply(1, jnp.concatenate([c1[:, 0:128] + below[1], c1[:, 128:256] + below[4]], axis=1))
    c1 = c1_ref[1]
    y1_high = apply(1, jnp.concatenate([c1[:, 0:128], c1[:, 128:256] + above[1]], axis=1))
    y1_ref[0] = y1_low
    y1_ref[1] = y1_high
    first = apply(0, c0_ref[0] + below[0])
    last = apply(0, c0_ref[7] + above[0])
    y0_ref[0] = first
    y0_ref[7] = last
    down = pack(first, y1_low[:, 0:128], y2[:, 0:128], y3, y1_low[:, 128:256], y2[:, 128:256])
    for t, tile in enumerate(down):
        down_ref[:, t * LANES : t * LANES + LANES] = tile
    up = pack(last, y1_high[:, 128:256], y2[:, 128:256], y3)
    for t, tile in enumerate(up):
        up_ref[:, t * LANES : t * LANES + LANES] = tile
    for i in range(1, 7):
        y0_ref[i] = apply(0, c0_ref[i])


def middle_kernel(filt_ref, w0_ref, w_ref, ww_ref, y0_ref, y1_ref, y2_ref, y3_ref, below_ref, above_ref, far_ref, *rest):
    *outs, u_ref, hi_ref, lo_ref = rest
    flags = edge_flags()
    longitude_synthesis(y0_ref, y1_ref, y2_ref, y3_ref, below_ref, above_ref, far_ref, w0_ref, w_ref, ww_ref, u_ref)

    def chunk(c, carry):
        at = pl.ds(pl.multiple_of(c * 16, 16), 16)
        rows = latitude_synthesis(pick_at(u_ref, at), filt_ref, flags)
        store_split(hi_ref, lo_ref, latitude_analysis(rows, filt_ref, flags), at)
        return carry

    lax.fori_loop(0, 9, chunk, 0)
    longitude_analysis(hi_ref, lo_ref, w0_ref, w_ref, *outs)


def last_kernel(filt_ref, w0_ref, w_ref, ww_ref, y0_ref, y1_ref, y2_ref, y3_ref, below_ref, above_ref, far_ref, out_ref,
                u_ref):
    flags = edge_flags()
    longitude_synthesis(y0_ref, y1_ref, y2_ref, y3_ref, below_ref, above_ref, far_ref, w0_ref, w_ref, ww_ref, u_ref)

    def chunk(c, carry):
        at = pl.ds(pl.multiple_of(c * 16, 16), 16)
        rows = latitude_synthesis(pick_at(u_ref, at), filt_ref, flags)
        start = pl.multiple_of(c * (16 * ROWS), 16 * ROWS)
        for r, values in rows.items():
            out_ref[pl.ds(start + r, 16, stride=ROWS), :] = values
        return carry

    lax.fori_loop(0, 8, chunk, 0)
    rows = latitude_synthesis(pick_at(u_ref, slice(128, 144)), filt_ref, flags)
    for r, values in rows.items():
        out_ref[pl.ds(128 * ROWS + r, 8, stride=ROWS), :] = values[0:8]
        out_ref[136 * ROWS + r : 136 * ROWS + r + 1, :] = values[8:9]


def prepare_kernel(m_ref, after_ref, plain_ref, turned_ref, wide_ref):
    del after_ref
    levels = m_ref.shape[1]
    wide_ref[...] = jnp.zeros_like(wide_ref)
    for band in range(m_ref.shape[0]):
        wide_ref[0:levels, 0:levels] = m_ref[band]
        values = wide_ref[...]
        for ref, matrix in ((plain_ref, values), (turned_ref, values.T)):
            high, low = split(matrix[0:PAD])
            ref[band, 0:PAD, :] = high
            ref[band, PAD : 2 * PAD, :] = low


VMEM = pl.BlockSpec(memory_space=pltpu.VMEM)
SMEM = pl.BlockSpec(memory_space=pltpu.SMEM)
ANY = pl.BlockSpec(memory_space=pl.ANY)


def shapes(*items):
    return [jax.ShapeDtypeStruct(shape, dtype) for shape, dtype in items]


COEFFICIENTS = (((8, PAD, 256), F32), ((2, PAD, 256), F32), ((PAD, 256), F32), ((PAD, LANES), F32))
WIDE_FIRST = (((PAD, 512), F32), ((PAD, 384), F32), ((40, LANES), F32))
WIDE_SECOND = (((PAD, 384), F32), ((PAD, 512), F32), ((40, LANES), F32))
WEIGHTS = (((80, LANES), F32), ((256, 512), BF16), ((3, 256, 256), BF16), ((3, 256, 256), BF16))


def call(kernel, in_specs, outs, scratch, name, limit, flops):
    return pl.pallas_call(
        kernel,
        out_shape=shapes(*outs),
        in_specs=in_specs,
        out_specs=[VMEM] * len(outs),
        scratch_shapes=scratch,
        compiler_params=pltpu.CompilerParams(vmem_limit_bytes=limit * MIB),
        cost_estimate=pl.CostEstimate(flops=flops, bytes_accessed=8 * MIB, transcendentals=0),
        name=name,
    )


def shift(values, by):
    count = lax.axis_size("lat")
    return lax.ppermute(values, "lat", [(i, i + by) for i in range(count) if 0 <= i + by < count])


def on_device(increment, filter_taps, band_roots):
    levels, rows, columns = increment.shape
    flat = increment.reshape(levels * rows, columns)
    halves = [pltpu.VMEM((SLOTS, PAD, 256), BF16)] * 2
    spread = [pltpu.VMEM((SLOTS, PAD, 256), F32)]
    filt, w0, w, ww, *rest = call(
        first_kernel, [SMEM, VMEM], WEIGHTS + COEFFICIENTS + WIDE_FIRST, halves, "first", 24, 10**9
    )(filter_taps, flat)
    plain, turned = call(
        prepare_kernel, [VMEM, ANY], (((5, 2 * PAD, 256), BF16),) * 2, [pltpu.VMEM((256, 256), F32)], "prepare", 16, 10**9
    )(band_roots, rest[-1])
    weights = [filt, w0, w, ww]

    def exchange_sums(up, down, far):
        return shift(up, 1), shift(down, -1), shift(far, 2)

    def exchange_values(up, down, far):
        return shift(up, 1), shift(down, -1), shift(far, -2)

    def vertical(matrix, own, received):
        return call(
            vertical_kernel, [VMEM] * 8, COEFFICIENTS + WIDE_SECOND, [], "vertical", 24, 10**9
        )(matrix, *own, *received)

    own, wide = rest[:4], rest[4:]
    *own, up, down, far = vertical(plain, own, exchange_sums(*wide))
    *own, up, down, far = call(
        middle_kernel, [VMEM] * 11, COEFFICIENTS + WIDE_FIRST, spread + halves, "middle", 32, 10**9
    )(*weights, *own, *exchange_values(up, down, far))
    *own, up, down, far = vertical(turned, own, exchange_sums(up, down, far))
    (out,) = call(
        last_kernel, [VMEM] * 11, (((levels * rows, columns), F32),), spread, "last", 24, 10**9
    )(*weights, *own, *exchange_values(up, down, far))
    return out.reshape(levels, rows, columns)


def solution(mesh):
    placed = (P("member", "lat", None), P(), P())
    return jax.shard_map(
        on_device, mesh=mesh, in_specs=placed, out_specs=P("member", "lat", None), check_vma=False
    )
```

```python
import functools
import math

import jax
import jax.numpy as jnp
from jax import lax
from jax.experimental import pallas as pl
from jax.experimental.pallas import tpu as pltpu
from jax.sharding import PartitionSpec as P

LEVELS = 4
TAPS = 5
ROOT_TWO = math.sqrt(2.0)
F32 = jnp.float32
BF16 = jnp.bfloat16
MIB = 1024 * 1024

ROWS = 16
OWN = (8, 4, 2, 1)
FIRST = -1
LAST = (8, 5, 3, 2)
COUNT = (10, 7, 5, 4)
BASE = (0, 10, 17, 22)
SLOTS = 26
LANES = 128
PAD = 144
KPAD = 256


def dot(a, b):
    return lax.dot_general(a, b, (((1,), (0,)), ((), ())), preferred_element_type=F32)


def dot_t(a, b):
    return lax.dot_general(a, b, (((1,), (1,)), ((), ())), preferred_element_type=F32)


def split(values):
    high = values.astype(BF16)
    return high, (values - high.astype(F32)).astype(BF16)


def slot(level, index):
    return BASE[level] + index - FIRST


def lane_ids(rows):
    return lax.broadcasted_iota(jnp.int32, (rows, LANES), 1)


def write_filters(taps_ref, filt_ref):
    signs = (1.0, -1.0, 1.0, -1.0, 1.0)
    ones = jnp.full((1, LANES), 1.0, F32)
    for level in range(LEVELS):
        for way in range(2):
            low = [taps_ref[level, way, 0, k].astype(F32) * ones for k in range(TAPS)]
            high = [taps_ref[level, way, 1, k].astype(F32) * ones for k in range(TAPS)]
            low_scale = ROOT_TWO / functools.reduce(jnp.add, low)
            high_scale = 1.0 / jnp.sqrt(functools.reduce(jnp.add, [h * h for h in high]))
            row = (level * 2 + way) * 2 * TAPS
            for k in range(TAPS):
                filt_ref[row + k : row + k + 1, :] = low[k] * low_scale
                filt_ref[row + TAPS + k : row + TAPS + k + 1, :] = (signs[k] * high[k]) * high_scale


def coeffs(filt_ref, level, way, kind):
    row = ((level * 2 + way) * 2 + kind) * TAPS
    return [filt_ref[row + k : row + k + 1, :] for k in range(TAPS)]


def write_weights(filt_ref, w0_ref, w_ref, ww_ref):
    row = lax.broadcasted_iota(jnp.int32, (LANES, LANES), 0)
    lane = lax.broadcasted_iota(jnp.int32, (LANES, LANES), 1)
    composed = None
    for level in range(LEVELS):
        half = (LANES // 2) >> level
        low = coeffs(filt_ref, level, 1, 0)
        high = coeffs(filt_ref, level, 1, 1)
        is_low = lane < half
        tap = row - 2 * jnp.where(is_low, lane, lane - half) + 2
        inside = (lane < 2 * half) & (row < 2 * half)
        step = jnp.zeros((LANES, LANES), F32)
        for k in range(TAPS):
            chosen = jnp.where(is_low, low[k], high[k])
            step = jnp.where(inside & (tap == k), chosen, step)
        if composed is None:
            composed = step
        else:
            composed = lax.dot_general(
                composed, step, (((1,), (0,)), ((), ())),
                precision=lax.Precision.HIGHEST, preferred_element_type=F32,
            )
        zeros = jnp.zeros((LANES, LANES), BF16)
        if level == 0:
            d_high, d_low = split(composed)
            moved = jnp.where(lane < half, pltpu.roll(composed, LANES - half, 1), 0.0)
            a_high, a_low = split(moved)
            w0_ref[0:LANES, 0:128] = zeros
            w0_ref[0:LANES, 128:256] = a_high
            w0_ref[0:LANES, 256:384] = zeros
            w0_ref[0:LANES, 384:512] = a_low
            w0_ref[LANES:256, 0:128] = d_high
            w0_ref[LANES:256, 128:256] = zeros
            w0_ref[LANES:256, 256:384] = d_low
            w0_ref[LANES:256, 384:512] = zeros
        else:
            moved = jnp.where((lane >= 2 * half) & (lane < 3 * half), pltpu.roll(composed, half, 1), 0.0)
            if level == LEVELS - 1:
                moved = moved + jnp.where(
                    (lane >= 3 * half) & (lane < 4 * half), pltpu.roll(composed, 3 * half, 1), 0.0
                )
            for part, values in ((0, moved), (1, composed)):
                rows = slice(part * LANES, part * LANES + LANES)
                v_high, v_low = split(values)
                w_ref[level - 1, rows, 0:128] = v_high
                w_ref[level - 1, rows, 128:256] = v_low
                ww_ref[level - 1, rows, 0:128] = v_high
                ww_ref[level - 1, rows, 128:256] = v_high


def edge_flags():
    place = lax.axis_index("lat")
    count = lax.axis_size("lat")
    lower = jnp.where(place == 0, 0.0, 1.0).astype(F32)
    upper = jnp.where(place == count - 1, 0.0, 1.0).astype(F32)
    return lower, upper


def masked(values, index, own, flags):
    if index < 0:
        return values * flags[0]
    if index >= own:
        return values * flags[1]
    return values


def latitude_analysis(rows, filt_ref, flags):
    out = {}
    for level in range(LEVELS):
        low = coeffs(filt_ref, level, 0, 0)
        high = coeffs(filt_ref, level, 0, 1)
        smooth = {}
        for index in range(FIRST, LAST[level] + 1):
            a = d = None
            for k in range(TAPS):
                source = rows.get(2 * index - 2 + k)
                if source is None:
                    continue
                a = low[k] * source if a is None else a + low[k] * source
                d = high[k] * source if d is None else d + high[k] * source
            if level < LEVELS - 1:
                a = masked(a, index, OWN[level], flags)
            smooth[index] = a
            out[slot(level, index)] = (a, d)
        rows = smooth
    return out


def latitude_synthesis(pick, filt_ref, flags):
    rows = None
    for level in reversed(range(LEVELS)):
        low = coeffs(filt_ref, level, 0, 0)
        high = coeffs(filt_ref, level, 0, 1)
        first, last = (FIRST, LAST[level - 1]) if level else (0, ROWS - 1)
        smooth, sharp = {}, {}
        for index in range(FIRST, LAST[level] + 1):
            a, d = pick(slot(level, index))
            smooth[index] = a if rows is None else a + rows[index]
            sharp[index] = d
        out = {}
        for r in range(first, last + 1):
            total = None
            for index in range(FIRST, LAST[level] + 1):
                k = r - 2 * index + 2
                if 0 <= k < TAPS:
                    term = low[k] * smooth[index] + high[k] * sharp[index]
                    total = term if total is None else total + term
            out[r] = masked(total, r, OWN[level - 1], flags) if level else total
        rows = out
    return rows


def pack(c0, c1, c2, c3, c1b, c2b):
    lane = lane_ids(PAD)
    return [
        c0[:, 0:128],
        jnp.where(lane < 64, c0[:, 128:256], jnp.where(lane < 112, pltpu.roll(c2, 64, 1), pltpu.roll(c2b, 80, 1))),
        jnp.where(lane < 96, c1, pltpu.roll(c3, 96, 1)),
        jnp.where(lane < 96, c1b, pltpu.roll(c2b, 96, 1)),
    ]


def unpack(tiles):
    parts = [
        jnp.concatenate([tiles[0], tiles[1]], axis=1),
        tiles[2],
        pltpu.roll(tiles[1], 64, 1),
        pltpu.roll(tiles[2], 32, 1),
    ]
    if len(tiles) > 3:
        lane = lane_ids(PAD)
        parts += [tiles[3], jnp.where(lane < 32, pltpu.roll(tiles[3], 32, 1), pltpu.roll(tiles[1], 48, 1))]
    return parts


def pack_coarse(c3):
    lane = lane_ids(40)
    last = jnp.concatenate([c3[120:144], jnp.zeros((16, LANES), F32)], axis=0)
    return jnp.where(
        lane < 32,
        c3[0:40],
        jnp.where(
            lane < 64,
            pltpu.roll(c3[40:80], 32, 1),
            jnp.where(lane < 96, pltpu.roll(c3[80:120], 64, 1), pltpu.roll(last, 96, 1)),
        ),
    )


def unpack_coarse(ref):
    values = ref[...]
    parts = [values] + [pltpu.roll(values, LANES - 32 * q, 1) for q in (1, 2, 3)]
    return jnp.concatenate(parts[:3] + [parts[3][0:24]], axis=0)


def is_even():
    return lax.rem(lax.axis_index("lat"), 2) == 0


def put(ref, tiles):
    for t, tile in enumerate(tiles):
        ref[t * PAD : t * PAD + PAD, :] = tile


def received(mate_ref, side_ref, n_below, n_above):
    even = is_even()
    place = lax.axis_index("lat")
    no_below = place == 0
    no_above = place == lax.axis_size("lat") - 1
    below, above = [], []
    for t in range(max(n_below, n_above)):
        mate = mate_ref[t * PAD : t * PAD + PAD, :]
        side = side_ref[t * PAD : t * PAD + PAD, :]
        if t < n_below:
            below.append(jnp.where(no_below, 0.0, jnp.where(even, side, mate)))
        if t < n_above:
            above.append(jnp.where(no_above, 0.0, jnp.where(even, mate, side)))
    return below, above


def store_split(hi_ref, lo_ref, out, at):
    for place, (a, d) in out.items():
        for part, values in ((0, a), (1, d)):
            lanes = slice(part * LANES, part * LANES + LANES)
            high, low = split(values)
            hi_ref[place, at, lanes] = high
            lo_ref[place, at, lanes] = low


def bands(hi_ref, lo_ref, w0_ref, w_ref):
    def level0(s):
        w_high, w_low = w0_ref[:, 0:256], w0_ref[:, 256:512]
        high = hi_ref[s]
        return dot(high, w_high) + dot(high, w_low) + dot(lo_ref[s], w_high)

    def others(level, s):
        both = dot(hi_ref[s], w_ref[level - 1])
        return both[:, 0:128] + both[:, 128:256] + dot(lo_ref[s], w_ref[level - 1, :, 0:128])

    return level0, others


def sums_message(hi_ref, lo_ref, w0_ref, w_ref, upward):
    level0, others = bands(hi_ref, lo_ref, w0_ref, w_ref)

    def chosen(level, up_index):
        return jnp.where(upward, slot(level, up_index), slot(level, -1))

    return pack(
        level0(chosen(0, 8)),
        others(1, chosen(1, 4)),
        others(2, chosen(2, 2)),
        others(3, chosen(3, 1)),
        others(1, slot(1, 5)),
        others(2, slot(2, 3)),
    )


def apply_vertical(m_ref, band, values):
    high, low = split(values)
    zeros = jnp.zeros((KPAD - PAD, values.shape[1]), BF16)
    high = jnp.concatenate([high, zeros], axis=0)
    low = jnp.concatenate([low, zeros], axis=0)
    both = dot(m_ref[band], high)
    return both[0:PAD] + both[PAD:] + dot(m_ref[band, 0:PAD], low)


def spread_level0(values, w0_ref):
    high, low = split(values)
    w_high, w_low = w0_ref[:, 0:256], w0_ref[:, 256:512]
    return dot_t(high, w_high) + dot_t(low, w_high) + dot_t(high, w_low)


def spread_other(level, values, w_ref, ww_ref):
    high, low = split(values)
    pair = jnp.concatenate([high, low], axis=1)
    return dot_t(pair, ww_ref[level - 1]) + dot_t(high, w_ref[level - 1, :, 128:256])


OWN_BASE = (0, 8, 12, 14)
GOT = {(0, -1): 0, (0, 8): 1, (1, -1): 2, (1, 4): 3, (1, 5): 4, (2, -1): 5, (2, 2): 6, (2, 3): 7, (3, -1): 8, (3, 1): 9, (3, 2): 10}


def spread_received(mate_ref, side_ref, far_ref, w0_ref, w_ref, ww_ref, got_ref):
    below, above = received(mate_ref, side_ref, 3, 4)
    below, above = unpack(below), unpack(above)
    far = unpack_coarse(far_ref)
    values = {(0, -1): below[0], (0, 8): above[0], (1, -1): below[1], (1, 4): above[1], (1, 5): above[4],
              (2, -1): below[2], (2, 2): above[2], (2, 3): above[5], (3, -1): below[3], (3, 1): above[3], (3, 2): far}
    for (level, index), v in values.items():
        if level == 0:
            got_ref[GOT[level, index]] = spread_level0(v, w0_ref)
        else:
            got_ref[GOT[level, index]] = spread_other(level, v, w_ref, ww_ref)


def pick_at(own_ref, got_ref, at):
    table = {}
    for level in range(LEVELS):
        for index in range(FIRST, LAST[level] + 1):
            if 0 <= index < OWN[level]:
                table[slot(level, index)] = (own_ref, OWN_BASE[level] + index)
            else:
                table[slot(level, index)] = (got_ref, GOT[level, index])

    def pick(place):
        ref, i = table[place]
        return ref[i, at, 0:128], ref[i, at, 128:256]

    return pick


def first_kernel(taps_ref, x_hbm, filt_ref, w0_ref, w_ref, ww_ref, hi_ref, lo_ref, side_ref, x_ref, sem):
    fetch = pltpu.make_async_copy(x_hbm, x_ref, sem)
    fetch.start()
    write_filters(taps_ref, filt_ref)
    flags = edge_flags()
    write_weights(filt_ref, w0_ref, w_ref, ww_ref)
    fetch.wait()

    def chunk(c, carry):
        start = pl.multiple_of(c * (16 * ROWS), 16 * ROWS)
        rows = {r: x_ref[pl.ds(start + r, 16, stride=ROWS), :] for r in range(ROWS)}
        at = pl.ds(pl.multiple_of(c * 16, 16), 16)
        store_split(hi_ref, lo_ref, latitude_analysis(rows, filt_ref, flags), at)
        return carry

    lax.fori_loop(0, 8, chunk, 0)
    top = lax.broadcasted_iota(jnp.int32, (8, LANES), 0) == 0
    rows = {}
    for r in range(ROWS):
        head = x_ref[pl.ds(128 * ROWS + r, 8, stride=ROWS), :]
        tail = jnp.where(top, x_ref[136 * ROWS + r : 136 * ROWS + r + 1, :], 0.0)
        rows[r] = jnp.concatenate([head, tail], axis=0)
    store_split(hi_ref, lo_ref, latitude_analysis(rows, filt_ref, flags), slice(128, 144))
    put(side_ref, sums_message(hi_ref, lo_ref, w0_ref, w_ref, jnp.logical_not(is_even())))


def mate_kernel(hi_ref, lo_ref, w0_ref, w_ref, mate_ref, far_ref):
    put(mate_ref, sums_message(hi_ref, lo_ref, w0_ref, w_ref, is_even()))
    _, others = bands(hi_ref, lo_ref, w0_ref, w_ref)
    far_ref[...] = pack_coarse(others(3, slot(3, 2)))


def own_kernel(hi_ref, lo_ref, w0_ref, w_ref, m_ref, c0_ref, c1_ref, c1b_ref, c2_ref, c3_ref, y0_ref, y1_ref):
    level0, others = bands(hi_ref, lo_ref, w0_ref, w_ref)
    c0_ref[0] = level0(slot(0, 0))
    c0_ref[1] = level0(slot(0, 7))
    c1_ref[:, 0:128] = others(1, slot(1, 0))
    c1_ref[:, 128:256] = others(1, slot(1, 1))
    c1b_ref[...] = others(1, slot(1, 3))
    c2_ref[:, 0:128] = others(2, slot(2, 0))
    c2_ref[:, 128:256] = others(2, slot(2, 1))
    c3_ref[...] = others(3, slot(3, 0))
    y1_ref[...] = apply_vertical(m_ref, 1, others(1, slot(1, 2)))
    for i in range(1, 7):
        y0_ref[i - 1] = apply_vertical(m_ref, 0, level0(slot(0, i)))


def vertical_kernel(m_ref, c0_ref, c1_ref, c1b_ref, c2_ref, c3_ref, mate_ref, side_ref, far_ref,
                    y0_ref, y1_ref, y1b_ref, y2_ref, y3_ref, mate_out_ref, side_out_ref, far_out_ref):
    below, above = received(mate_ref, side_ref, 4, 3)
    below, above = unpack(below), unpack(above)
    far = unpack_coarse(far_ref)
    c3 = c3_ref[...] + below[3] + above[3] + far
    lane = lane_ids(PAD)
    y3 = jnp.where(lane < 24, apply_vertical(m_ref, 3, c3), apply_vertical(m_ref, 4, c3))
    c2 = c2_ref[...]
    y2 = apply_vertical(m_ref, 2, jnp.concatenate([c2[:, 0:128] + below[2], c2[:, 128:256] + below[5] + above[2]], axis=1))
    c1 = c1_ref[...]
    y1 = apply_vertical(m_ref, 1, jnp.concatenate([c1[:, 0:128] + below[1], c1[:, 128:256] + below[4]], axis=1))
    y1b = apply_vertical(m_ref, 1, c1b_ref[...] + above[1])
    first = apply_vertical(m_ref, 0, c0_ref[0] + below[0])
    last = apply_vertical(m_ref, 0, c0_ref[1] + above[0])
    y0_ref[0] = first
    y0_ref[1] = last
    y1_ref[...] = y1
    y1b_ref[...] = y1b
    y2_ref[...] = y2
    y3_ref[...] = y3
    far_out_ref[...] = pack_coarse(y3)
    down = pack(first, y1[:, 0:128], y2[:, 0:128], y3, y1[:, 128:256], y2[:, 128:256])
    up = pack(last, y1b, y2[:, 128:256], y3, y1[:, 128:256], y2[:, 128:256])
    even = is_even()
    put(side_out_ref, [jnp.where(even, d, u) for d, u in zip(down, up)])
    put(mate_out_ref, [jnp.where(even, u, d) for d, u in zip(down, up)])


def spread_kernel(w0_ref, w_ref, ww_ref, y0c_ref, y1c_ref, y0_ref, y1_ref, y1b_ref, y2_ref, y3_ref, own_ref):
    for i in range(8):
        values = y0_ref[i // 7] if i in (0, 7) else y0c_ref[i - 1]
        own_ref[i] = spread_level0(values, w0_ref)
    for i, values in enumerate((y1_ref[:, 0:128], y1_ref[:, 128:256], y1c_ref[...], y1b_ref[...])):
        own_ref[8 + i] = spread_other(1, values, w_ref, ww_ref)
    for i in range(2):
        own_ref[12 + i] = spread_other(2, y2_ref[:, i * 128 : i * 128 + 128], w_ref, ww_ref)
    own_ref[14] = spread_other(3, y3_ref[...], w_ref, ww_ref)


def middle_kernel(filt_ref, w0_ref, w_ref, ww_ref, own_ref, mate_ref, side_ref, far_ref, hi_ref, lo_ref, side_out_ref,
                  got_ref):
    flags = edge_flags()
    spread_received(mate_ref, side_ref, far_ref, w0_ref, w_ref, ww_ref, got_ref)

    def chunk(c, carry):
        at = pl.ds(pl.multiple_of(c * 16, 16), 16)
        rows = latitude_synthesis(pick_at(own_ref, got_ref, at), filt_ref, flags)
        store_split(hi_ref, lo_ref, latitude_analysis(rows, filt_ref, flags), at)
        return carry

    lax.fori_loop(0, 9, chunk, 0)
    put(side_out_ref, sums_message(hi_ref, lo_ref, w0_ref, w_ref, jnp.logical_not(is_even())))


def last_kernel(filt_ref, w0_ref, w_ref, ww_ref, own_ref, mate_ref, side_ref, far_ref, out_hbm, got_ref, out_ref, sems):
    flags = edge_flags()
    spread_received(mate_ref, side_ref, far_ref, w0_ref, w_ref, ww_ref, got_ref)

    def leave(c):
        part = pl.ds(pl.multiple_of(c * (16 * ROWS), 16 * ROWS), 16 * ROWS)
        return pltpu.make_async_copy(out_ref.at[part, :], out_hbm.at[part, :], sems.at[c])

    def chunk(c, carry):
        at = pl.ds(pl.multiple_of(c * 16, 16), 16)
        rows = latitude_synthesis(pick_at(own_ref, got_ref, at), filt_ref, flags)
        start = pl.multiple_of(c * (16 * ROWS), 16 * ROWS)
        for r, values in rows.items():
            out_ref[pl.ds(start + r, 16, stride=ROWS), :] = values
        leave(c).start()
        return carry

    lax.fori_loop(0, 8, chunk, 0)
    rows = latitude_synthesis(pick_at(own_ref, got_ref, slice(128, 144)), filt_ref, flags)
    for r, values in rows.items():
        out_ref[pl.ds(128 * ROWS + r, 8, stride=ROWS), :] = values[0:8]
        out_ref[136 * ROWS + r : 136 * ROWS + r + 1, :] = values[8:9]
    rest = pl.ds(128 * ROWS, 9 * ROWS)
    tail = pltpu.make_async_copy(out_ref.at[rest, :], out_hbm.at[rest, :], sems.at[8])
    tail.start()
    for c in range(8):
        leave(c).wait()
    tail.wait()


def prepare_kernel(m_ref, after_ref, plain_ref, turned_ref, wide_ref):
    del after_ref
    levels = m_ref.shape[1]
    wide_ref[...] = jnp.zeros_like(wide_ref)
    for band in range(m_ref.shape[0]):
        wide_ref[0:levels, 0:levels] = m_ref[band]
        values = wide_ref[...]
        for ref, matrix in ((plain_ref, values), (turned_ref, values.T)):
            high, low = split(matrix[0:PAD])
            ref[band, 0:PAD, :] = high
            ref[band, PAD : 2 * PAD, :] = low


VMEM = pl.BlockSpec(memory_space=pltpu.VMEM)
SMEM = pl.BlockSpec(memory_space=pltpu.SMEM)
HBM = pl.BlockSpec(memory_space=pltpu.HBM)
ANY = pl.BlockSpec(memory_space=pl.ANY)

MESSAGE = ((4 * PAD, LANES), F32)
FAR = ((40, LANES), F32)
WEIGHTS = (((80, LANES), F32), ((256, 512), BF16), ((3, 256, 256), BF16), ((3, 256, 256), BF16))
HALVES = (((SLOTS, PAD, 256), BF16),) * 2
EDGES = (((2, PAD, 256), F32), ((PAD, 256), F32), ((PAD, LANES), F32), ((PAD, 256), F32), ((PAD, LANES), F32))
INNER = (((6, PAD, 256), F32), ((PAD, LANES), F32))
OWN_WIDE = ((15, PAD, 256), F32)
GOT_WIDE = pltpu.VMEM((11, PAD, 256), F32)


def call(kernel, in_specs, outs, scratch, name, limit, out_spec=VMEM):
    return pl.pallas_call(
        kernel,
        out_shape=[jax.ShapeDtypeStruct(shape, dtype) for shape, dtype in outs],
        in_specs=in_specs,
        out_specs=[out_spec] * len(outs),
        scratch_shapes=scratch,
        compiler_params=pltpu.CompilerParams(vmem_limit_bytes=limit * MIB),
        cost_estimate=pl.CostEstimate(flops=10**9, bytes_accessed=8 * MIB, transcendentals=0),
        name=name,
    )


def swap(values, phase):
    count = lax.axis_size("lat")
    partner = {}
    for i in range(phase, count - 1, 2):
        partner[i], partner[i + 1] = i + 1, i
    return lax.ppermute(values, "lat", [(i, partner.get(i, i)) for i in range(count)])


def shift(values, by):
    count = lax.axis_size("lat")
    return lax.ppermute(values, "lat", [(i, i + by) for i in range(count) if 0 <= i + by < count])


def on_device(increment, filter_taps, band_roots):
    levels, rows, columns = increment.shape
    flat = increment.reshape(levels * rows, columns)
    filt, w0, w, ww, hi, lo, side = call(
        first_kernel, [SMEM, HBM], WEIGHTS + HALVES + (MESSAGE,),
        [pltpu.VMEM((levels * rows, columns), F32), pltpu.SemaphoreType.DMA], "first", 16,
    )(filter_taps, flat)
    plain, turned = call(
        prepare_kernel, [VMEM, ANY], (((5, 2 * PAD, 256), BF16),) * 2, [pltpu.VMEM((256, 256), F32)], "prepare", 12
    )(band_roots, side)

    def half(matrix, hi, lo, side):
        side = swap(side, 1)
        mate, far = call(mate_kernel, [VMEM] * 4, (MESSAGE, FAR), [], "mate", 12)(hi, lo, w0, w)
        mate, far = swap(mate, 0), shift(far, 2)
        *edges, y0c, y1c = call(own_kernel, [VMEM] * 5, EDGES + INNER, [], "own", 12)(hi, lo, w0, w, matrix)
        *edges, mate, side, far = call(
            vertical_kernel, [VMEM] * 9, EDGES + (MESSAGE, MESSAGE, FAR), [], "vertical", 12
        )(matrix, *edges, mate, side, far)
        side, mate, far = swap(side, 1), swap(mate, 0), shift(far, -2)
        (own,) = call(spread_kernel, [VMEM] * 10, (OWN_WIDE,), [], "spread", 12)(w0, w, ww, y0c, y1c, *edges)
        return filt, w0, w, ww, own, mate, side, far

    hi, lo, side = call(middle_kernel, [VMEM] * 8, HALVES + (MESSAGE,), [GOT_WIDE], "middle", 16)(
        *half(plain, hi, lo, side)
    )
    (out,) = call(
        last_kernel, [VMEM] * 8, (((levels * rows, columns), F32),),
        [GOT_WIDE, pltpu.VMEM((levels * rows, columns), F32), pltpu.SemaphoreType.DMA((9,))], "last", 16, HBM,
    )(*half(turned, hi, lo, side))
    return out.reshape(levels, rows, columns)


def solution(mesh):
    placed = (P("member", "lat", None), P(), P())
    return jax.shard_map(
        on_device, mesh=mesh, in_specs=placed, out_specs=P("member", "lat", None), check_vma=False
    )
```

```python
import functools
import math

import jax
import jax.numpy as jnp
from jax import lax
from jax.experimental import pallas as pl
from jax.experimental.pallas import tpu as pltpu
from jax.sharding import PartitionSpec as P


LEVELS = 4
TAPS = 5
ROOT_TWO = math.sqrt(2.0)
F32 = jnp.float32
BF16 = jnp.bfloat16
MIB = 1024 * 1024

ROWS = 16
OWN = (8, 4, 2, 1)
FIRST = -1
LAST = (8, 5, 3, 2)
BASE = (0, 10, 17, 22)
SLOTS = 26
LANES = 128
PAD = 144
KPAD = 256


def dot(a, b):
    return lax.dot_general(a, b, (((1,), (0,)), ((), ())), preferred_element_type=F32)


def dot_t(a, b):
    return lax.dot_general(a, b, (((1,), (1,)), ((), ())), preferred_element_type=F32)


def split(values):
    high = values.astype(BF16)
    return high, (values - high.astype(F32)).astype(BF16)


def slot(level, index):
    return BASE[level] + index - FIRST


def lane_ids(rows):
    return lax.broadcasted_iota(jnp.int32, (rows, LANES), 1)


def write_filters(taps_ref, filt_ref):
    signs = (1.0, -1.0, 1.0, -1.0, 1.0)
    ones = jnp.full((1, LANES), 1.0, F32)
    for level in range(LEVELS):
        for way in range(2):
            low = [taps_ref[level, way, 0, k].astype(F32) * ones for k in range(TAPS)]
            high = [taps_ref[level, way, 1, k].astype(F32) * ones for k in range(TAPS)]
            low_scale = ROOT_TWO / functools.reduce(jnp.add, low)
            high_scale = 1.0 / jnp.sqrt(functools.reduce(jnp.add, [h * h for h in high]))
            row = (level * 2 + way) * 2 * TAPS
            for k in range(TAPS):
                filt_ref[row + k : row + k + 1, :] = low[k] * low_scale
                filt_ref[row + TAPS + k : row + TAPS + k + 1, :] = (signs[k] * high[k]) * high_scale


def coeffs(filt_ref, level, way, kind):
    row = ((level * 2 + way) * 2 + kind) * TAPS
    return [filt_ref[row + k : row + k + 1, :] for k in range(TAPS)]


def write_weights(filt_ref, w0_ref, w_ref, ww_ref):
    row = lax.broadcasted_iota(jnp.int32, (LANES, LANES), 0)
    lane = lax.broadcasted_iota(jnp.int32, (LANES, LANES), 1)
    composed = None
    for level in range(LEVELS):
        half = (LANES // 2) >> level
        low = coeffs(filt_ref, level, 1, 0)
        high = coeffs(filt_ref, level, 1, 1)
        is_low = lane < half
        tap = row - 2 * jnp.where(is_low, lane, lane - half) + 2
        inside = (lane < 2 * half) & (row < 2 * half)
        step = jnp.zeros((LANES, LANES), F32)
        for k in range(TAPS):
            chosen = jnp.where(is_low, low[k], high[k])
            step = jnp.where(inside & (tap == k), chosen, step)
        if composed is None:
            composed = step
        else:
            composed = lax.dot_general(
                composed, step, (((1,), (0,)), ((), ())),
                precision=lax.Precision.HIGHEST, preferred_element_type=F32,
            )
        zeros = jnp.zeros((LANES, LANES), BF16)
        if level == 0:
            d_high, d_low = split(composed)
            moved = jnp.where(lane < half, pltpu.roll(composed, LANES - half, 1), 0.0)
            a_high, a_low = split(moved)
            w0_ref[0:LANES, 0:128] = zeros
            w0_ref[0:LANES, 128:256] = a_high
            w0_ref[0:LANES, 256:384] = zeros
            w0_ref[0:LANES, 384:512] = a_low
            w0_ref[LANES:256, 0:128] = d_high
            w0_ref[LANES:256, 128:256] = zeros
            w0_ref[LANES:256, 256:384] = d_low
            w0_ref[LANES:256, 384:512] = zeros
        else:
            moved = jnp.where((lane >= 2 * half) & (lane < 3 * half), pltpu.roll(composed, half, 1), 0.0)
            if level == LEVELS - 1:
                moved = moved + jnp.where(
                    (lane >= 3 * half) & (lane < 4 * half), pltpu.roll(composed, 3 * half, 1), 0.0
                )
            for part, values in ((0, moved), (1, composed)):
                rows = slice(part * LANES, part * LANES + LANES)
                v_high, v_low = split(values)
                w_ref[level - 1, rows, 0:128] = v_high
                w_ref[level - 1, rows, 128:256] = v_low
                ww_ref[level - 1, rows, 0:128] = v_high
                ww_ref[level - 1, rows, 128:256] = v_high


def edge_flags():
    place = lax.axis_index("lat")
    count = lax.axis_size("lat")
    lower = jnp.where(place == 0, 0.0, 1.0).astype(F32)
    upper = jnp.where(place == count - 1, 0.0, 1.0).astype(F32)
    return lower, upper


def masked(values, index, own, flags):
    if index < 0:
        return values * flags[0]
    if index >= own:
        return values * flags[1]
    return values


def latitude_analysis(rows, filt_ref, flags):
    out = {}
    for level in range(LEVELS):
        low = coeffs(filt_ref, level, 0, 0)
        high = coeffs(filt_ref, level, 0, 1)
        smooth = {}
        for index in range(FIRST, LAST[level] + 1):
            a = d = None
            for k in range(TAPS):
                source = rows.get(2 * index - 2 + k)
                if source is None:
                    continue
                a = low[k] * source if a is None else a + low[k] * source
                d = high[k] * source if d is None else d + high[k] * source
            if level < LEVELS - 1:
                a = masked(a, index, OWN[level], flags)
            smooth[index] = a
            out[slot(level, index)] = (a, d)
        rows = smooth
    return out


def latitude_synthesis(pick, filt_ref, flags):
    rows = None
    for level in reversed(range(LEVELS)):
        low = coeffs(filt_ref, level, 0, 0)
        high = coeffs(filt_ref, level, 0, 1)
        first, last = (FIRST, LAST[level - 1]) if level else (0, ROWS - 1)
        smooth, sharp = {}, {}
        for index in range(FIRST, LAST[level] + 1):
            a, d = pick(slot(level, index))
            smooth[index] = a if rows is None else a + rows[index]
            sharp[index] = d
        out = {}
        for r in range(first, last + 1):
            total = None
            for index in range(FIRST, LAST[level] + 1):
                k = r - 2 * index + 2
                if 0 <= k < TAPS:
                    term = low[k] * smooth[index] + high[k] * sharp[index]
                    total = term if total is None else total + term
            out[r] = masked(total, r, OWN[level - 1], flags) if level else total
        rows = out
    return rows


def pack(c0, c1, c2, c3, c1b, c2b):
    lane = lane_ids(PAD)
    return [
        c0[:, 0:128],
        jnp.where(lane < 64, c0[:, 128:256], jnp.where(lane < 112, pltpu.roll(c2, 64, 1), pltpu.roll(c2b, 80, 1))),
        jnp.where(lane < 96, c1, pltpu.roll(c3, 96, 1)),
        jnp.where(lane < 96, c1b, pltpu.roll(c2b, 96, 1)),
    ]


def unpack(tiles):
    parts = [
        jnp.concatenate([tiles[0], tiles[1]], axis=1),
        tiles[2],
        pltpu.roll(tiles[1], 64, 1),
        pltpu.roll(tiles[2], 32, 1),
    ]
    if len(tiles) > 3:
        lane = lane_ids(PAD)
        parts += [tiles[3], jnp.where(lane < 32, pltpu.roll(tiles[3], 32, 1), pltpu.roll(tiles[1], 48, 1))]
    return parts


def pack_coarse(c3):
    lane = lane_ids(40)
    last = jnp.concatenate([c3[120:144], jnp.zeros((16, LANES), F32)], axis=0)
    return jnp.where(
        lane < 32,
        c3[0:40],
        jnp.where(
            lane < 64,
            pltpu.roll(c3[40:80], 32, 1),
            jnp.where(lane < 96, pltpu.roll(c3[80:120], 64, 1), pltpu.roll(last, 96, 1)),
        ),
    )


def unpack_coarse(values):
    parts = [values] + [pltpu.roll(values, LANES - 32 * q, 1) for q in (1, 2, 3)]
    return jnp.concatenate(parts[:3] + [parts[3][0:24]], axis=0)


def is_even():
    return lax.rem(lax.axis_index("lat"), 2) == 0


AT = (0, PAD, 3 * PAD, 2 * PAD)
COARSE = slice(4 * PAD, 4 * PAD + 40)


def part(ref, t):
    return ref[AT[t] : AT[t] + PAD, :]


def put(ref, tiles):
    for t, tile in enumerate(tiles):
        ref[AT[t] : AT[t] + PAD, :] = tile


def received(mate_ref, side_ref, n_below, n_above):
    even = is_even()
    place = lax.axis_index("lat")
    no_below = place == 0
    no_above = place == lax.axis_size("lat") - 1
    below, above = [], []
    for t in range(max(n_below, n_above)):
        mate, side = part(mate_ref, t), part(side_ref, t)
        if t < n_below:
            below.append(jnp.where(no_below, 0.0, jnp.where(even, side, mate)))
        if t < n_above:
            above.append(jnp.where(no_above, 0.0, jnp.where(even, mate, side)))
    return below, above


def store_split(hi_ref, lo_ref, out, at):
    for place, (a, d) in out.items():
        for part, values in ((0, a), (1, d)):
            lanes = slice(part * LANES, part * LANES + LANES)
            high, low = split(values)
            hi_ref[place, at, lanes] = high
            lo_ref[place, at, lanes] = low


def bands(hi_ref, lo_ref, w0_ref, w_ref):
    def level0(s):
        w_high, w_low = w0_ref[:, 0:256], w0_ref[:, 256:512]
        high = hi_ref[s]
        return dot(high, w_high) + dot(high, w_low) + dot(lo_ref[s], w_high)

    def others(level, s):
        both = dot(hi_ref[s], w_ref[level - 1])
        return both[:, 0:128] + both[:, 128:256] + dot(lo_ref[s], w_ref[level - 1, :, 0:128])

    return level0, others


def sums_message(hi_ref, lo_ref, w0_ref, w_ref, upward):
    level0, others = bands(hi_ref, lo_ref, w0_ref, w_ref)

    def chosen(level, up_index):
        return jnp.where(upward, slot(level, up_index), slot(level, -1))

    return pack(
        level0(chosen(0, 8)),
        others(1, chosen(1, 4)),
        others(2, chosen(2, 2)),
        others(3, chosen(3, 1)),
        others(1, slot(1, 5)),
        others(2, slot(2, 3)),
    )


def apply_vertical(m_ref, band, values):
    high, low = split(values)
    zeros = jnp.zeros((KPAD - PAD, values.shape[1]), BF16)
    high = jnp.concatenate([high, zeros], axis=0)
    low = jnp.concatenate([low, zeros], axis=0)
    both = dot(m_ref[band], high)
    return both[0:PAD] + both[PAD:] + dot(m_ref[band, 0:PAD], low)


def spread_level0(values, w0_ref):
    high, low = split(values)
    w_high, w_low = w0_ref[:, 0:256], w0_ref[:, 256:512]
    return dot_t(high, w_high) + dot_t(low, w_high) + dot_t(high, w_low)


def spread_other(level, values, w_ref, ww_ref):
    high, low = split(values)
    pair = jnp.concatenate([high, low], axis=1)
    return dot_t(pair, ww_ref[level - 1]) + dot_t(high, w_ref[level - 1, :, 128:256])


OWN_BASE = (0, 8, 12, 14)
GOT = {(0, -1): 0, (0, 8): 1, (1, -1): 2, (1, 4): 3, (1, 5): 4, (2, -1): 5, (2, 2): 6, (2, 3): 7, (3, -1): 8, (3, 1): 9}


def pick_at(own_ref, got_ref, far_ref, at):
    table = {}
    for level in range(LEVELS):
        for index in range(FIRST, LAST[level] + 1):
            if 0 <= index < OWN[level]:
                table[slot(level, index)] = (own_ref, OWN_BASE[level] + index)
            elif (level, index) in GOT:
                table[slot(level, index)] = (got_ref, GOT[level, index])
            else:
                table[slot(level, index)] = (far_ref, 0)

    def pick(place):
        ref, i = table[place]
        return ref[i, at, 0:128], ref[i, at, 128:256]

    return pick


def weights_kernel(taps_ref, filt_ref, w0_ref, w_ref, ww_ref):
    write_filters(taps_ref, filt_ref)
    write_weights(filt_ref, w0_ref, w_ref, ww_ref)


def first_kernel(filt_ref, x_ref, hi_ref, lo_ref):
    flags = edge_flags()

    def chunk(c, carry):
        start = pl.multiple_of(c * (16 * ROWS), 16 * ROWS)
        rows = {r: x_ref[pl.ds(start + r, 16, stride=ROWS), :] for r in range(ROWS)}
        at = pl.ds(pl.multiple_of(c * 16, 16), 16)
        store_split(hi_ref, lo_ref, latitude_analysis(rows, filt_ref, flags), at)
        return carry

    lax.fori_loop(0, 8, chunk, 0)
    top = lax.broadcasted_iota(jnp.int32, (8, LANES), 0) == 0
    rows = {}
    for r in range(ROWS):
        head = x_ref[pl.ds(128 * ROWS + r, 8, stride=ROWS), :]
        tail = jnp.where(top, x_ref[136 * ROWS + r : 136 * ROWS + r + 1, :], 0.0)
        rows[r] = jnp.concatenate([head, tail], axis=0)
    store_split(hi_ref, lo_ref, latitude_analysis(rows, filt_ref, flags), slice(128, 144))


def side_kernel(hi_ref, lo_ref, w0_ref, w_ref, side_ref, far_ref):
    put(side_ref, sums_message(hi_ref, lo_ref, w0_ref, w_ref, jnp.logical_not(is_even())))
    _, others = bands(hi_ref, lo_ref, w0_ref, w_ref)
    far = pack_coarse(others(3, slot(3, 2)))
    far_ref[...] = far
    side_ref[COARSE, :] = far


def mate_kernel(hi_ref, lo_ref, w0_ref, w_ref, after_ref, mate_ref):
    del after_ref
    even = is_even()
    tiles = sums_message(hi_ref, lo_ref, w0_ref, w_ref, even)
    _, others = bands(hi_ref, lo_ref, w0_ref, w_ref)
    tiles[3] = jnp.where(even, tiles[3], others(3, slot(3, 0)))
    put(mate_ref, tiles)


def own_kernel(hi_ref, lo_ref, w0_ref, w_ref, m_ref, c0_ref, c1_ref, c1b_ref, c2_ref, c3_ref, c3up_ref, y0_ref, y1_ref):
    level0, others = bands(hi_ref, lo_ref, w0_ref, w_ref)
    c0_ref[0] = level0(slot(0, 0))
    c0_ref[1] = level0(slot(0, 7))
    c1_ref[:, 0:128] = others(1, slot(1, 0))
    c1_ref[:, 128:256] = others(1, slot(1, 1))
    c1b_ref[...] = others(1, slot(1, 3))
    c2_ref[:, 0:128] = others(2, slot(2, 0))
    c2_ref[:, 128:256] = others(2, slot(2, 1))
    c3_ref[...] = others(3, slot(3, 0))
    c3up_ref[...] = others(3, slot(3, 1))
    y1_ref[...] = apply_vertical(m_ref, 1, others(1, slot(1, 2)))
    for i in range(1, 7):
        y0_ref[i - 1] = apply_vertical(m_ref, 0, level0(slot(0, i)))


def vertical_kernel(m_ref, c0_ref, c1_ref, c1b_ref, c2_ref, mate_ref, side_ref,
                    y0_ref, y1_ref, y1b_ref, y2_ref, mate_out_ref, side_out_ref):
    below, above = received(mate_ref, side_ref, 4, 3)
    below, above = unpack(below), unpack(above)
    c2 = c2_ref[...]
    y2 = apply_vertical(m_ref, 2, jnp.concatenate([c2[:, 0:128] + below[2], c2[:, 128:256] + below[5] + above[2]], axis=1))
    c1 = c1_ref[...]
    y1 = apply_vertical(m_ref, 1, jnp.concatenate([c1[:, 0:128] + below[1], c1[:, 128:256] + below[4]], axis=1))
    y1b = apply_vertical(m_ref, 1, c1b_ref[...] + above[1])
    first = apply_vertical(m_ref, 0, c0_ref[0] + below[0])
    last = apply_vertical(m_ref, 0, c0_ref[1] + above[0])
    y0_ref[0] = first
    y0_ref[1] = last
    y1_ref[...] = y1
    y1b_ref[...] = y1b
    y2_ref[...] = y2
    none = jnp.zeros((PAD, LANES), F32)
    down = pack(first, y1[:, 0:128], y2[:, 0:128], none, y1[:, 128:256], y2[:, 128:256])
    up = pack(last, y1b, y2[:, 128:256], none, y1[:, 128:256], y2[:, 128:256])
    even = is_even()
    put(side_out_ref, [jnp.where(even, d, u) for d, u in zip(down, up)])
    put(mate_out_ref, [jnp.where(even, u, d) for d, u in zip(down, up)])


def coarse_kernel(m_ref, c3_ref, c3up_ref, far_ref, mate_ref, side_ref, passed_ref, mate_in_ref, side_in_ref,
                  y3_ref, mate_out_ref, side_out_ref):
    even = is_even()
    place = lax.axis_index("lat")
    last = lax.axis_size("lat") - 1
    lane = lane_ids(PAD)
    from_side = jnp.where((place == 0) | (place == last), 0.0, pltpu.roll(part(side_ref, 2), 32, 1))
    passed = unpack_coarse(passed_ref[PAD : PAD + 40, :])
    passed = jnp.where(even, unpack_coarse(far_ref[...]), jnp.where(place == 1, 0.0, passed))
    mine = c3_ref[...] + pltpu.roll(part(mate_ref, 2), 32, 1) + from_side + passed
    coarse = jnp.where(place == 0, 0.0, unpack_coarse(side_ref[COARSE, :]))
    above = jnp.where(place == last - 1, 0.0, pltpu.roll(passed_ref[0:PAD, :], 32, 1))
    other = part(mate_ref, 3) + c3up_ref[...] + coarse + above
    both = jnp.concatenate([mine, other], axis=1)
    detail, smooth = apply_vertical(m_ref, 3, both), apply_vertical(m_ref, 4, both)
    y3 = jnp.where(lane < 24, detail[:, 0:128], smooth[:, 0:128])
    y3_ref[...] = y3
    moved = pltpu.roll(y3, 96, 1)
    mate_out_ref[...] = mate_in_ref[...]
    mate_out_ref[AT[2] : AT[2] + PAD, :] = jnp.where(lane < 96, part(mate_in_ref, 2), moved)
    side_out_ref[0 : 4 * PAD, :] = side_in_ref[...]
    side_out_ref[AT[2] : AT[2] + PAD, :] = jnp.where(lane < 96, part(side_in_ref, 2), moved)
    side_out_ref[COARSE, :] = pack_coarse(jnp.where(lane < 24, detail[:, 128:256], smooth[:, 128:256]))


def spread_kernel(w0_ref, w_ref, ww_ref, y0c_ref, y1c_ref, y0_ref, y1_ref, y1b_ref, y2_ref, y3_ref, own_ref):
    for i in range(8):
        values = y0_ref[i // 7] if i in (0, 7) else y0c_ref[i - 1]
        own_ref[i] = spread_level0(values, w0_ref)
    for i, values in enumerate((y1_ref[:, 0:128], y1_ref[:, 128:256], y1c_ref[...], y1b_ref[...])):
        own_ref[8 + i] = spread_other(1, values, w_ref, ww_ref)
    for i in range(2):
        own_ref[12 + i] = spread_other(2, y2_ref[:, i * 128 : i * 128 + 128], w_ref, ww_ref)
    own_ref[14] = spread_other(3, y3_ref[...], w_ref, ww_ref)


def received_kernel(w0_ref, w_ref, ww_ref, mate_ref, side_ref, got_ref):
    below, above = received(mate_ref, side_ref, 3, 4)
    below, above = unpack(below), unpack(above)
    values = {(0, -1): below[0], (0, 8): above[0], (1, -1): below[1], (1, 4): above[1], (1, 5): above[4],
              (2, -1): below[2], (2, 2): above[2], (2, 3): above[5], (3, -1): below[3], (3, 1): above[3]}
    for (level, index), v in values.items():
        if level == 0:
            got_ref[GOT[level, index]] = spread_level0(v, w0_ref)
        else:
            got_ref[GOT[level, index]] = spread_other(level, v, w_ref, ww_ref)


def spread_coarse(side_ref, passed_ref, w_ref, ww_ref, far_ref):
    value = jnp.where(is_even(), pltpu.roll(passed_ref[...], 32, 1), unpack_coarse(side_ref[COARSE, :]))
    value = jnp.where(lax.axis_index("lat") >= lax.axis_size("lat") - 2, 0.0, value)
    far_ref[0] = spread_other(3, value, w_ref, ww_ref)


def middle_kernel(filt_ref, w_ref, ww_ref, own_ref, got_ref, side_ref, passed_ref, hi_ref, lo_ref, far_ref):
    flags = edge_flags()
    spread_coarse(side_ref, passed_ref, w_ref, ww_ref, far_ref)

    def chunk(c, carry):
        at = pl.ds(pl.multiple_of(c * 16, 16), 16)
        rows = latitude_synthesis(pick_at(own_ref, got_ref, far_ref, at), filt_ref, flags)
        store_split(hi_ref, lo_ref, latitude_analysis(rows, filt_ref, flags), at)
        return carry

    lax.fori_loop(0, 9, chunk, 0)


def last_kernel(filt_ref, w_ref, ww_ref, own_ref, got_ref, side_ref, passed_ref, out_hbm, far_ref, out_ref, sems):
    flags = edge_flags()
    spread_coarse(side_ref, passed_ref, w_ref, ww_ref, far_ref)

    def leave(c):
        piece = pl.ds(pl.multiple_of(c * (16 * ROWS), 16 * ROWS), 16 * ROWS)
        return pltpu.make_async_copy(out_ref.at[piece, :], out_hbm.at[piece, :], sems.at[c])

    def chunk(c, carry):
        at = pl.ds(pl.multiple_of(c * 16, 16), 16)
        rows = latitude_synthesis(pick_at(own_ref, got_ref, far_ref, at), filt_ref, flags)
        start = pl.multiple_of(c * (16 * ROWS), 16 * ROWS)
        for r, values in rows.items():
            out_ref[pl.ds(start + r, 16, stride=ROWS), :] = values
        leave(c).start()
        return carry

    lax.fori_loop(0, 8, chunk, 0)
    rows = latitude_synthesis(pick_at(own_ref, got_ref, far_ref, slice(128, 144)), filt_ref, flags)
    for r, values in rows.items():
        out_ref[pl.ds(128 * ROWS + r, 8, stride=ROWS), :] = values[0:8]
        out_ref[136 * ROWS + r : 136 * ROWS + r + 1, :] = values[8:9]
    rest = pl.ds(128 * ROWS, 9 * ROWS)
    tail = pltpu.make_async_copy(out_ref.at[rest, :], out_hbm.at[rest, :], sems.at[8])
    tail.start()
    for c in range(8):
        leave(c).wait()
    tail.wait()


def prepare_kernel(m_ref, after_ref, plain_ref, turned_ref, wide_ref):
    del after_ref
    levels = m_ref.shape[1]
    wide_ref[...] = jnp.zeros_like(wide_ref)
    for band in range(m_ref.shape[0]):
        wide_ref[0:levels, 0:levels] = m_ref[band]
        values = wide_ref[...]
        for ref, matrix in ((plain_ref, values), (turned_ref, values.T)):
            high, low = split(matrix[0:PAD])
            ref[band, 0:PAD, :] = high
            ref[band, PAD : 2 * PAD, :] = low


VMEM = pl.BlockSpec(memory_space=pltpu.VMEM)
SMEM = pl.BlockSpec(memory_space=pltpu.SMEM)
HBM = pl.BlockSpec(memory_space=pltpu.HBM)
ANY = pl.BlockSpec(memory_space=pl.ANY)

MESSAGE = ((4 * PAD, LANES), F32)
SIDE = ((4 * PAD + 40, LANES), F32)
FAR = ((40, LANES), F32)
WEIGHTS = (((80, LANES), F32), ((256, 512), BF16), ((3, 256, 256), BF16), ((3, 256, 256), BF16))
HALVES = (((SLOTS, PAD, 256), BF16),) * 2
EDGES = (((2, PAD, 256), F32), ((PAD, 256), F32), ((PAD, LANES), F32), ((PAD, 256), F32))
COARSEST = ((PAD, LANES), F32)
INNER = (((6, PAD, 256), F32), ((PAD, LANES), F32))
OWN_WIDE = ((15, PAD, 256), F32)
GOT_WIDE = ((10, PAD, 256), F32)
FAR_WIDE = pltpu.VMEM((1, PAD, 256), F32)


def call(kernel, in_specs, outs, scratch, limit, out_spec=VMEM):
    return pl.pallas_call(
        kernel,
        out_shape=[jax.ShapeDtypeStruct(shape, dtype) for shape, dtype in outs],
        in_specs=in_specs,
        out_specs=[out_spec] * len(outs),
        scratch_shapes=scratch,
        compiler_params=pltpu.CompilerParams(vmem_limit_bytes=limit * MIB),
        cost_estimate=pl.CostEstimate(flops=10**9, bytes_accessed=8 * MIB, transcendentals=0),
    )


def swap(values, phase):
    count = lax.axis_size("lat")
    partner = {}
    for i in range(phase, count - 1, 2):
        partner[i], partner[i + 1] = i + 1, i
    return lax.ppermute(values, "lat", [(i, partner.get(i, i)) for i in range(count)])


def pass_up(values):
    count = lax.axis_size("lat")
    return lax.ppermute(values, "lat", [(i, i + 2) for i in range(0, count - 2, 2)])


def on_device(increment, filter_taps, band_roots):
    levels, rows, columns = increment.shape
    flat = increment.reshape(levels * rows, columns)
    filt, w0, w, ww = call(weights_kernel, [SMEM], WEIGHTS, [], 12)(filter_taps)
    hi, lo = call(first_kernel, [VMEM] * 2, HALVES, [], 12)(filt, flat)
    plain, turned = call(
        prepare_kernel, [VMEM, ANY], (((5, 2 * PAD, 256), BF16),) * 2, [pltpu.VMEM((256, 256), F32)], 12
    )(band_roots, hi)

    def half(matrix, hi, lo):
        side, far = call(side_kernel, [VMEM] * 4, (SIDE, FAR), [], 12)(hi, lo, w0, w)
        (mate,) = call(mate_kernel, [VMEM] * 4 + [ANY], (MESSAGE,), [], 12)(hi, lo, w0, w, side)
        side, mate, far = swap(side, 1), swap(mate, 0), pass_up(far)
        *edges, c3, c3up, y0c, y1c = call(
            own_kernel, [VMEM] * 5, EDGES + (COARSEST, COARSEST) + INNER, [], 12
        )(hi, lo, w0, w, matrix)
        side, y1c = lax.optimization_barrier((side, y1c))
        passed = swap(side[3 * PAD :], 0)
        *edges, mate_out, side_out = call(
            vertical_kernel, [VMEM] * 7, EDGES + (MESSAGE, MESSAGE), [], 12
        )(matrix, *edges, mate, side)
        y3, mate, side = call(coarse_kernel, [VMEM] * 9, (COARSEST, MESSAGE, SIDE), [], 12)(
            matrix, c3, c3up, far, mate, side, passed, mate_out, side_out
        )
        side, mate = swap(side, 1), swap(mate, 0)
        (own,) = call(spread_kernel, [VMEM] * 10, (OWN_WIDE,), [], 12)(w0, w, ww, y0c, y1c, *edges, y3)
        side, own = lax.optimization_barrier((side, own))
        passed = swap(side[3 * PAD : 4 * PAD], 0)
        (got,) = call(received_kernel, [VMEM] * 5, (GOT_WIDE,), [], 12)(w0, w, ww, mate, side)
        return filt, w, ww, own, got, side, passed

    ready = half(plain, hi, lo)
    hi, lo = call(middle_kernel, [VMEM] * 7, HALVES, [FAR_WIDE], 12)(*ready)
    ready = half(turned, hi, lo)
    (out,) = call(
        last_kernel, [VMEM] * 7, (((levels * rows, columns), F32),),
        [FAR_WIDE, pltpu.VMEM((levels * rows, columns), F32), pltpu.SemaphoreType.DMA((9,))], 12, HBM,
    )(*ready)
    return out.reshape(levels, rows, columns)


def solution(mesh):
    placed = (P("member", "lat", None), P(), P())
    return jax.shard_map(
        on_device, mesh=mesh, in_specs=placed, out_specs=P("member", "lat", None), check_vma=False
    )
```

```python
import functools
import math

import jax
import jax.numpy as jnp
from jax import lax
from jax.experimental import pallas as pl
from jax.experimental.pallas import tpu as pltpu
from jax.sharding import PartitionSpec as P


LEVELS = 4
TAPS = 5
ROOT_TWO = math.sqrt(2.0)
F32 = jnp.float32
BF16 = jnp.bfloat16
MIB = 1024 * 1024

ROWS = 16
OWN = (8, 4, 2, 1)
FIRST = -1
LAST = (8, 5, 3, 2)
BASE = (0, 10, 17, 22)
SLOTS = 26
LANES = 128
PAD = 144
KPAD = 256


def dot(a, b):
    return lax.dot_general(a, b, (((1,), (0,)), ((), ())), preferred_element_type=F32)


def dot_t(a, b):
    return lax.dot_general(a, b, (((1,), (1,)), ((), ())), preferred_element_type=F32)


def split(values):
    high = values.astype(BF16)
    return high, (values - high.astype(F32)).astype(BF16)


def slot(level, index):
    return BASE[level] + index - FIRST


def lane_ids(rows):
    return lax.broadcasted_iota(jnp.int32, (rows, LANES), 1)


def write_filters(taps_ref, filt_ref):
    signs = (1.0, -1.0, 1.0, -1.0, 1.0)
    ones = jnp.full((1, LANES), 1.0, F32)
    for level in range(LEVELS):
        for way in range(2):
            low = [taps_ref[level, way, 0, k].astype(F32) * ones for k in range(TAPS)]
            high = [taps_ref[level, way, 1, k].astype(F32) * ones for k in range(TAPS)]
            low_scale = ROOT_TWO / functools.reduce(jnp.add, low)
            high_scale = 1.0 / jnp.sqrt(functools.reduce(jnp.add, [h * h for h in high]))
            row = (level * 2 + way) * 2 * TAPS
            for k in range(TAPS):
                filt_ref[row + k : row + k + 1, :] = low[k] * low_scale
                filt_ref[row + TAPS + k : row + TAPS + k + 1, :] = (signs[k] * high[k]) * high_scale


def coeffs(filt_ref, level, way, kind):
    row = ((level * 2 + way) * 2 + kind) * TAPS
    return [filt_ref[row + k : row + k + 1, :] for k in range(TAPS)]


def product(a, b):
    a_high, a_low = split(a)
    b_high, b_low = split(b)
    return dot(a_high, b_high) + dot(a_low, b_high) + dot(a_high, b_low)


def write_weights(filt_ref, w0_ref, w_ref, ww_ref):
    row = lax.broadcasted_iota(jnp.int32, (LANES, LANES), 0)
    lane = lax.broadcasted_iota(jnp.int32, (LANES, LANES), 1)
    steps = []
    for level in range(LEVELS):
        half = (LANES // 2) >> level
        low = coeffs(filt_ref, level, 1, 0)
        high = coeffs(filt_ref, level, 1, 1)
        is_low = lane < half
        tap = row - 2 * jnp.where(is_low, lane, lane - half) + 2
        inside = (lane < 2 * half) & (row < 2 * half)
        step = jnp.zeros((LANES, LANES), F32)
        for k in range(TAPS):
            chosen = jnp.where(is_low[0:1], low[k], high[k])
            step = jnp.where(tap == k, chosen, step)
        steps.append(jnp.where(inside, step, 0.0))
    second = product(steps[0], steps[1])
    composed_steps = [steps[0], second, product(second, steps[2]), product(second, product(steps[2], steps[3]))]
    zeros = jnp.zeros((LANES, LANES), BF16)
    for level, composed in enumerate(composed_steps):
        half = (LANES // 2) >> level
        if level == 0:
            d_high, d_low = split(composed)
            moved = jnp.where(lane < half, pltpu.roll(composed, LANES - half, 1), 0.0)
            a_high, a_low = split(moved)
            w0_ref[0:LANES, 0:128] = zeros
            w0_ref[0:LANES, 128:256] = a_high
            w0_ref[0:LANES, 256:384] = zeros
            w0_ref[0:LANES, 384:512] = a_low
            w0_ref[LANES:256, 0:128] = d_high
            w0_ref[LANES:256, 128:256] = zeros
            w0_ref[LANES:256, 256:384] = d_low
            w0_ref[LANES:256, 384:512] = zeros
        else:
            moved = jnp.where((lane >= 2 * half) & (lane < 3 * half), pltpu.roll(composed, half, 1), 0.0)
            if level == LEVELS - 1:
                moved = moved + jnp.where(
                    (lane >= 3 * half) & (lane < 4 * half), pltpu.roll(composed, 3 * half, 1), 0.0
                )
            for which, values in ((0, moved), (1, composed)):
                rows = slice(which * LANES, which * LANES + LANES)
                v_high, v_low = split(values)
                w_ref[level - 1, rows, 0:128] = v_high
                w_ref[level - 1, rows, 128:256] = v_low
                ww_ref[level - 1, rows, 0:128] = v_high
                ww_ref[level - 1, rows, 128:256] = v_high


def edge_flags():
    place = lax.axis_index("lat")
    count = lax.axis_size("lat")
    lower = jnp.where(place == 0, 0.0, 1.0).astype(F32)
    upper = jnp.where(place == count - 1, 0.0, 1.0).astype(F32)
    return lower, upper


def masked(values, index, own, flags):
    if index < 0:
        return values * flags[0]
    if index >= own:
        return values * flags[1]
    return values


def latitude_analysis(rows, filt_ref, flags):
    out = {}
    for level in range(LEVELS):
        low = coeffs(filt_ref, level, 0, 0)
        high = coeffs(filt_ref, level, 0, 1)
        smooth = {}
        for index in range(FIRST, LAST[level] + 1):
            a = d = None
            for k in range(TAPS):
                source = rows.get(2 * index - 2 + k)
                if source is None:
                    continue
                a = low[k] * source if a is None else a + low[k] * source
                d = high[k] * source if d is None else d + high[k] * source
            if level < LEVELS - 1:
                a = masked(a, index, OWN[level], flags)
            smooth[index] = a
            out[slot(level, index)] = (a, d)
        rows = smooth
    return out


def latitude_synthesis(pick, filt_ref, flags):
    rows = None
    for level in reversed(range(LEVELS)):
        low = coeffs(filt_ref, level, 0, 0)
        high = coeffs(filt_ref, level, 0, 1)
        first, last = (FIRST, LAST[level - 1]) if level else (0, ROWS - 1)
        smooth, sharp = {}, {}
        for index in range(FIRST, LAST[level] + 1):
            a, d = pick(slot(level, index))
            smooth[index] = a if rows is None else a + rows[index]
            sharp[index] = d
        out = {}
        for r in range(first, last + 1):
            total = None
            for index in range(FIRST, LAST[level] + 1):
                k = r - 2 * index + 2
                if 0 <= k < TAPS:
                    term = low[k] * smooth[index] + high[k] * sharp[index]
                    total = term if total is None else total + term
            out[r] = masked(total, r, OWN[level - 1], flags) if level else total
        rows = out
    return rows


def pack(c0, c1, c2, c3, c1b, c2b, c3b=None):
    lane = lane_ids(PAD)
    last = jnp.where(lane < 64, c1b, pltpu.roll(c2b, 96, 1))
    if c3b is not None:
        last = with_far(last, c3b)
    return [
        c0[:, 0:128],
        jnp.where(lane < 64, c0[:, 128:256], jnp.where(lane < 112, pltpu.roll(c2, 64, 1), pltpu.roll(c2b, 80, 1))),
        jnp.where(lane < 96, c1, pltpu.roll(c3, 96, 1)),
        last,
    ]


def with_far(tile, c3b):
    lane = lane_ids(PAD)
    return jnp.where((lane >= 64) & (lane < 96), pltpu.roll(c3b, 64, 1), tile)


def far_of(tile):
    return pltpu.roll(tile, 64, 1)


def unpack(tiles):
    parts = [
        jnp.concatenate([tiles[0], tiles[1]], axis=1),
        tiles[2],
        pltpu.roll(tiles[1], 64, 1),
        pltpu.roll(tiles[2], 32, 1),
    ]
    if len(tiles) > 3:
        lane = lane_ids(PAD)
        parts += [tiles[3], jnp.where(lane < 32, pltpu.roll(tiles[3], 32, 1), pltpu.roll(tiles[1], 48, 1))]
    return parts


def three_bands(tile, filt_ref):
    low, high = coeffs(filt_ref, 1, 0, 0)[0], coeffs(filt_ref, 1, 0, 1)[0]
    return jnp.where(lane_ids(PAD) < 64, high * tile, pltpu.roll(low * tile, 32, 1))


def two_sums(values, filt_ref):
    ratio = coeffs(filt_ref, 1, 0, 1)[0] / coeffs(filt_ref, 1, 0, 0)[0]
    return jnp.where(lane_ids(PAD) < 32, values, pltpu.roll(values, 96, 1) + ratio * values)


def bands_of_sums(tile):
    lane = lane_ids(PAD)
    return jnp.where(lane < 32, tile, jnp.where(lane < 64, 0.0, pltpu.roll(tile, 32, 1)))


def pack_coarse(c3):
    lane = lane_ids(40)
    last = jnp.concatenate([c3[120:144], jnp.zeros((16, LANES), F32)], axis=0)
    return jnp.where(
        lane < 32,
        c3[0:40],
        jnp.where(
            lane < 64,
            pltpu.roll(c3[40:80], 32, 1),
            jnp.where(lane < 96, pltpu.roll(c3[80:120], 64, 1), pltpu.roll(last, 96, 1)),
        ),
    )


def unpack_coarse(values):
    parts = [values] + [pltpu.roll(values, LANES - 32 * q, 1) for q in (1, 2, 3)]
    return jnp.concatenate(parts[:3] + [parts[3][0:24]], axis=0)


def is_even():
    return lax.rem(lax.axis_index("lat"), 2) == 0


MAIN = 136
ORDERED = (0, 1, 3, 2)
ENDS = 4 * MAIN
TAIL = 2 * MAIN
END_TILE = 3 * MAIN


def join(main, end):
    top = lax.broadcasted_iota(jnp.int32, (8, LANES), 0) == 0
    return jnp.concatenate([main, jnp.where(top, end, 0.0)], axis=0)


def part(ref, t, start=0):
    at = ORDERED[t] * MAIN - start
    end = ENDS + t - start
    return join(ref[at : at + MAIN, :], ref[end : end + 1, :])


def put_one(ref, t, tile):
    ref[ORDERED[t] * MAIN : ORDERED[t] * MAIN + MAIN, :] = tile[0:MAIN]
    ref[ENDS + t : ENDS + t + 1, :] = tile[MAIN : MAIN + 1]


def put(ref, tiles):
    ref[ENDS : ENDS + 8, :] = jnp.zeros((8, LANES), F32)
    for t, tile in enumerate(tiles):
        put_one(ref, t, tile)


def received(mate_ref, side_ref, n_below, n_above):
    even = is_even()
    place = lax.axis_index("lat")
    no_below = place == 0
    no_above = place == lax.axis_size("lat") - 1
    below, above = [], []
    for t in range(max(n_below, n_above)):
        mate, side = part(mate_ref, t), part(side_ref, t)
        if t < n_below:
            below.append(jnp.where(no_below, 0.0, jnp.where(even, side, mate)))
        if t < n_above:
            above.append(jnp.where(no_above, 0.0, jnp.where(even, mate, side)))
    return below, above


def store_split(hi_ref, lo_ref, out, at):
    for place, (a, d) in out.items():
        for part, values in ((0, a), (1, d)):
            lanes = slice(part * LANES, part * LANES + LANES)
            high, low = split(values)
            hi_ref[place, at, lanes] = high
            lo_ref[place, at, lanes] = low


def stack(parts):
    return jnp.concatenate(parts, axis=0)


def bands(hi_ref, lo_ref, w0_ref, w_ref):
    def level0(*slots):
        w_high, w_low = w0_ref[:, 0:256], w0_ref[:, 256:512]
        high, low = stack([hi_ref[s] for s in slots]), stack([lo_ref[s] for s in slots])
        out = dot(high, w_high) + dot(high, w_low) + dot(low, w_high)
        return [out[i * PAD : i * PAD + PAD] for i in range(len(slots))]

    def others(level, *slots):
        high, low = stack([hi_ref[s] for s in slots]), stack([lo_ref[s] for s in slots])
        both = dot(high, w_ref[level - 1])
        out = both[:, 0:128] + both[:, 128:256] + dot(low, w_ref[level - 1, :, 0:128])
        return [out[i * PAD : i * PAD + PAD] for i in range(len(slots))]

    return level0, others


def sums_message(hi_ref, lo_ref, w0_ref, w_ref, upward, extra):
    level0, others = bands(hi_ref, lo_ref, w0_ref, w_ref)

    def chosen(level, up_index):
        return jnp.where(upward, slot(level, up_index), slot(level, -1))

    (c0,) = level0(chosen(0, 8))
    (c1,) = others(1, chosen(1, 4))
    row = slot(0, 8)
    both = dot(hi_ref[row, :, 0:128], w_ref[0, 128:256, :])
    c1b = both[:, 0:128] + both[:, 128:256] + dot(lo_ref[row, :, 0:128], w_ref[0, 128:256, 0:128])
    c2, c2b = others(2, chosen(2, 2), slot(2, 3))
    c3, more = others(3, chosen(3, 1), slot(3, extra))
    return pack(c0, c1, c2, c3, c1b, c2b, more), more


def apply_vertical(m_ref, band, values):
    high, low = split(values)
    zeros = jnp.zeros((KPAD - PAD, values.shape[1]), BF16)
    high = jnp.concatenate([high, zeros], axis=0)
    low = jnp.concatenate([low, zeros], axis=0)
    both = dot(m_ref[band], high)
    return both[0:PAD] + both[PAD:] + dot(m_ref[band, 0:PAD], low)


def spread_level0(values, w0_ref):
    high, low = split(stack(values))
    w_high, w_low = w0_ref[:, 0:256], w0_ref[:, 256:512]
    out = dot_t(high, w_high) + dot_t(low, w_high) + dot_t(high, w_low)
    return [out[i * PAD : i * PAD + PAD] for i in range(len(values))]


def spread_other(level, values, w_ref, ww_ref):
    high, low = split(stack(values))
    pair = jnp.concatenate([high, low], axis=1)
    out = dot_t(pair, ww_ref[level - 1]) + dot_t(high, w_ref[level - 1, :, 128:256])
    return [out[i * PAD : i * PAD + PAD] for i in range(len(values))]


OWN_BASE = (0, 8, 12, 14)
GOT = {(0, -1): 0, (0, 8): 1, (1, -1): 2, (1, 4): 3, (1, 5): 4, (2, -1): 5, (2, 2): 6, (2, 3): 7, (3, -1): 8, (3, 1): 9}


def pick_at(own_ref, got_ref, far_ref, at):
    table = {}
    for level in range(LEVELS):
        for index in range(FIRST, LAST[level] + 1):
            if 0 <= index < OWN[level]:
                table[slot(level, index)] = (own_ref, OWN_BASE[level] + index)
            elif (level, index) in GOT:
                table[slot(level, index)] = (got_ref, GOT[level, index])
            else:
                table[slot(level, index)] = (far_ref, 0)

    def pick(place):
        ref, i = table[place]
        return ref[i, at, 0:128], ref[i, at, 128:256]

    return pick


def weights_kernel(taps_ref, filt_ref, w0_ref, w_ref, ww_ref):
    write_filters(taps_ref, filt_ref)
    write_weights(filt_ref, w0_ref, w_ref, ww_ref)


def first_kernel(filt_ref, x_ref, hi_ref, lo_ref):
    flags = edge_flags()

    def chunk(c, carry):
        start = pl.multiple_of(c * (16 * ROWS), 16 * ROWS)
        rows = {r: x_ref[pl.ds(start + r, 16, stride=ROWS), :] for r in range(ROWS)}
        at = pl.ds(pl.multiple_of(c * 16, 16), 16)
        store_split(hi_ref, lo_ref, latitude_analysis(rows, filt_ref, flags), at)
        return carry

    lax.fori_loop(0, 8, chunk, 0)
    top = lax.broadcasted_iota(jnp.int32, (8, LANES), 0) == 0
    rows = {}
    for r in range(ROWS):
        head = x_ref[pl.ds(128 * ROWS + r, 8, stride=ROWS), :]
        tail = jnp.where(top, x_ref[136 * ROWS + r : 136 * ROWS + r + 1, :], 0.0)
        rows[r] = jnp.concatenate([head, tail], axis=0)
    store_split(hi_ref, lo_ref, latitude_analysis(rows, filt_ref, flags), slice(128, 144))


def side_kernel(hi_ref, lo_ref, w0_ref, w_ref, side_ref, far_ref):
    tiles, share = sums_message(hi_ref, lo_ref, w0_ref, w_ref, jnp.logical_not(is_even()), 2)
    put(side_ref, tiles)
    far_ref[...] = pack_coarse(share)


def mate_kernel(hi_ref, lo_ref, w0_ref, w_ref, after_ref, mate_ref):
    del after_ref
    tiles, _ = sums_message(hi_ref, lo_ref, w0_ref, w_ref, is_even(), 0)
    put(mate_ref, tiles)


def own_kernel(hi_ref, lo_ref, w0_ref, w_ref, c0_ref, c1_ref, c1b_ref, c2_ref, c3_ref, c3up_ref):
    level0, others = bands(hi_ref, lo_ref, w0_ref, w_ref)
    c0_ref[0], c0_ref[1] = level0(slot(0, 0), slot(0, 7))
    c1_ref[:, 0:128], c1_ref[:, 128:256], c1b_ref[...] = others(1, slot(1, 0), slot(1, 1), slot(1, 3))
    c2_ref[:, 0:128], c2_ref[:, 128:256] = others(2, slot(2, 0), slot(2, 1))
    c3_ref[...], c3up_ref[...] = others(3, slot(3, 0), slot(3, 1))


def inner_kernel(hi_ref, lo_ref, w0_ref, w_ref, m_ref, after_ref, y0_ref, y1_ref):
    del after_ref
    level0, others = bands(hi_ref, lo_ref, w0_ref, w_ref)
    y1_ref[...] = apply_vertical(m_ref, 1, others(1, slot(1, 2))[0])
    for i, c0 in enumerate(level0(*[slot(0, i) for i in range(1, 7)])):
        y0_ref[i] = apply_vertical(m_ref, 0, c0)


def vertical_kernel(m_ref, filt_ref, c0_ref, c1_ref, c1b_ref, c2_ref, mate_ref, side_ref,
                    y0_ref, y1_ref, y1b_ref, y2_ref, mate_out_ref, side_out_ref):
    below, above = received(mate_ref, side_ref, 4, 3)
    below, above = unpack(below), unpack(above)
    c2 = c2_ref[...]
    y2 = apply_vertical(m_ref, 2, jnp.concatenate([c2[:, 0:128] + below[2], c2[:, 128:256] + below[5] + above[2]], axis=1))
    c1 = c1_ref[...]
    y1 = apply_vertical(m_ref, 1, jnp.concatenate([c1[:, 0:128] + below[1], c1[:, 128:256] + three_bands(below[4], filt_ref)], axis=1))
    y1b = apply_vertical(m_ref, 1, c1b_ref[...] + above[1])
    first = apply_vertical(m_ref, 0, c0_ref[0] + below[0])
    last = apply_vertical(m_ref, 0, c0_ref[1] + above[0])
    y0_ref[0] = first
    y0_ref[1] = last
    y1_ref[...] = y1
    y1b_ref[...] = y1b
    y2_ref[...] = y2
    none = jnp.zeros((PAD, LANES), F32)
    sums = two_sums(y1[:, 128:256], filt_ref)
    down = pack(first, y1[:, 0:128], y2[:, 0:128], none, sums, y2[:, 128:256])
    up = pack(last, y1b, y2[:, 128:256], none, sums, y2[:, 128:256])
    even = is_even()
    put(side_out_ref, [jnp.where(even, d, u) for d, u in zip(down, up)])
    put(mate_out_ref, [jnp.where(even, u, d) for d, u in zip(down, up)])


def coarse_kernel(m_ref, c3_ref, c3up_ref, far_ref, mate_ref, side_ref, passed_ref, mate_in_ref, side_in_ref,
                  y3_ref, mate_out_ref, side_out_ref):
    even = is_even()
    place = lax.axis_index("lat")
    last = lax.axis_size("lat") - 1
    lane = lane_ids(PAD)
    from_side = jnp.where((place == 0) | (place == last), 0.0, pltpu.roll(part(side_ref, 2), 32, 1))
    passed = far_of(part(passed_ref, 3, TAIL))
    passed = jnp.where(even, unpack_coarse(far_ref[...]), jnp.where(place == 1, 0.0, passed))
    mine = c3_ref[...] + pltpu.roll(part(mate_ref, 2), 32, 1) + from_side + passed
    coarse = jnp.where(place == 0, 0.0, far_of(part(side_ref, 3)))
    above = jnp.where(place == last - 1, 0.0, pltpu.roll(part(passed_ref, 2, TAIL), 32, 1))
    other = far_of(part(mate_ref, 3)) + c3up_ref[...] + coarse + above
    both = jnp.concatenate([mine, other], axis=1)
    detail, smooth = apply_vertical(m_ref, 3, both), apply_vertical(m_ref, 4, both)
    y3 = jnp.where(lane < 24, detail[:, 0:128], smooth[:, 0:128])
    y3_ref[...] = y3
    moved = pltpu.roll(y3, 96, 1)
    mate_out_ref[...] = mate_in_ref[...]
    put_one(mate_out_ref, 2, jnp.where(lane < 96, part(mate_in_ref, 2), moved))
    side_out_ref[...] = side_in_ref[...]
    put_one(side_out_ref, 2, jnp.where(lane < 96, part(side_in_ref, 2), moved))
    y3_other = jnp.where(lane < 24, detail[:, 128:256], smooth[:, 128:256])
    put_one(side_out_ref, 3, with_far(part(side_in_ref, 3), y3_other))


def spread_kernel(w0_ref, w_ref, ww_ref, y0c_ref, y1c_ref, y0_ref, y1_ref, y1b_ref, y2_ref, y3_ref, own_ref):
    level0 = [y0_ref[i // 7] if i in (0, 7) else y0c_ref[i - 1] for i in range(8)]
    level1 = [y1_ref[:, 0:128], y1_ref[:, 128:256], y1c_ref[...], y1b_ref[...]]
    level2 = [y2_ref[:, 0:128], y2_ref[:, 128:256]]
    wide = spread_level0(level0, w0_ref)
    for level, values in ((1, level1), (2, level2), (3, [y3_ref[...]])):
        wide += spread_other(level, values, w_ref, ww_ref)
    for i, values in enumerate(wide):
        own_ref[i] = values


def received_kernel(w0_ref, w_ref, ww_ref, mate_ref, side_ref, got_ref):
    below, above = received(mate_ref, side_ref, 3, 4)
    below, above = unpack(below), unpack(above)
    wide = spread_level0([below[0], above[0]], w0_ref)
    wide += spread_other(1, [below[1], above[1], bands_of_sums(above[4])], w_ref, ww_ref)
    wide += spread_other(2, [below[2], above[2], above[5]], w_ref, ww_ref)
    wide += spread_other(3, [below[3], above[3]], w_ref, ww_ref)
    for i, values in enumerate(wide):
        got_ref[i] = values


def spread_coarse(side_ref, passed_ref, w_ref, ww_ref, far_ref):
    value = jnp.where(is_even(), pltpu.roll(part(passed_ref, 2, END_TILE), 32, 1), far_of(part(side_ref, 3)))
    value = jnp.where(lax.axis_index("lat") >= lax.axis_size("lat") - 2, 0.0, value)
    far_ref[0] = spread_other(3, [value], w_ref, ww_ref)[0]


def middle_kernel(filt_ref, w_ref, ww_ref, own_ref, got_ref, side_ref, passed_ref, hi_ref, lo_ref, far_ref):
    flags = edge_flags()
    spread_coarse(side_ref, passed_ref, w_ref, ww_ref, far_ref)

    def chunk(c, carry):
        at = pl.ds(pl.multiple_of(c * 16, 16), 16)
        rows = latitude_synthesis(pick_at(own_ref, got_ref, far_ref, at), filt_ref, flags)
        store_split(hi_ref, lo_ref, latitude_analysis(rows, filt_ref, flags), at)
        return carry

    lax.fori_loop(0, 9, chunk, 0)


def last_kernel(filt_ref, w_ref, ww_ref, own_ref, got_ref, side_ref, passed_ref, out_hbm, far_ref, out_ref, sems):
    flags = edge_flags()
    spread_coarse(side_ref, passed_ref, w_ref, ww_ref, far_ref)

    def leave(c):
        piece = pl.ds(pl.multiple_of(c * (16 * ROWS), 16 * ROWS), 16 * ROWS)
        return pltpu.make_async_copy(out_ref.at[piece, :], out_hbm.at[piece, :], sems.at[c])

    def chunk(c, carry):
        at = pl.ds(pl.multiple_of(c * 16, 16), 16)
        rows = latitude_synthesis(pick_at(own_ref, got_ref, far_ref, at), filt_ref, flags)
        start = pl.multiple_of(c * (16 * ROWS), 16 * ROWS)
        for r, values in rows.items():
            out_ref[pl.ds(start + r, 16, stride=ROWS), :] = values
        leave(c).start()
        return carry

    lax.fori_loop(0, 8, chunk, 0)
    rows = latitude_synthesis(pick_at(own_ref, got_ref, far_ref, slice(128, 144)), filt_ref, flags)
    for r, values in rows.items():
        out_ref[pl.ds(128 * ROWS + r, 8, stride=ROWS), :] = values[0:8]
        out_ref[136 * ROWS + r : 136 * ROWS + r + 1, :] = values[8:9]
    rest = pl.ds(128 * ROWS, 9 * ROWS)
    tail = pltpu.make_async_copy(out_ref.at[rest, :], out_hbm.at[rest, :], sems.at[8])
    tail.start()
    for c in range(8):
        leave(c).wait()
    tail.wait()


def prepare_kernel(turned, m_ref, after_ref, out_ref, wide_ref):
    del after_ref
    levels = m_ref.shape[1]
    wide_ref[...] = jnp.zeros_like(wide_ref)
    for band in range(m_ref.shape[0]):
        wide_ref[0:levels, 0:levels] = m_ref[band]
        matrix = wide_ref[...].T if turned else wide_ref[...]
        high, low = split(matrix[0:PAD])
        out_ref[band, 0:PAD, :] = high
        out_ref[band, PAD : 2 * PAD, :] = low


VMEM = pl.BlockSpec(memory_space=pltpu.VMEM)
SMEM = pl.BlockSpec(memory_space=pltpu.SMEM)
HBM = pl.BlockSpec(memory_space=pltpu.HBM)
ANY = pl.BlockSpec(memory_space=pl.ANY)

MESSAGE = ((4 * MAIN + 8, LANES), F32)
FAR = ((40, LANES), F32)
WEIGHTS = (((80, LANES), F32), ((256, 512), BF16), ((3, 256, 256), BF16), ((3, 256, 256), BF16))
HALVES = (((SLOTS, PAD, 256), BF16),) * 2
EDGES = (((2, PAD, 256), F32), ((PAD, 256), F32), ((PAD, LANES), F32), ((PAD, 256), F32))
COARSEST = ((PAD, LANES), F32)
INNER = (((6, PAD, 256), F32), ((PAD, LANES), F32))
OWN_WIDE = ((15, PAD, 256), F32)
GOT_WIDE = ((10, PAD, 256), F32)
FAR_WIDE = pltpu.VMEM((1, PAD, 256), F32)


def call(kernel, in_specs, outs, scratch, limit, out_spec=VMEM):
    return pl.pallas_call(
        kernel,
        out_shape=[jax.ShapeDtypeStruct(shape, dtype) for shape, dtype in outs],
        in_specs=in_specs,
        out_specs=[out_spec] * len(outs),
        scratch_shapes=scratch,
        compiler_params=pltpu.CompilerParams(vmem_limit_bytes=limit * MIB),
        cost_estimate=pl.CostEstimate(flops=10**9, bytes_accessed=8 * MIB, transcendentals=0),
    )


def swap(values, phase):
    count = lax.axis_size("lat")
    partner = {}
    for i in range(phase, count - 1, 2):
        partner[i], partner[i + 1] = i + 1, i
    return lax.ppermute(values, "lat", [(i, partner.get(i, i)) for i in range(count)])


def pass_up(values):
    count = lax.axis_size("lat")
    return lax.ppermute(values, "lat", [(i, i + 2) for i in range(0, count - 2, 2)])


def on_device(increment, filter_taps, band_roots):
    levels, rows, columns = increment.shape
    flat = increment.reshape(levels * rows, columns)
    filt, w0, w, ww = call(weights_kernel, [SMEM], WEIGHTS, [], 12)(filter_taps)
    hi, lo = call(first_kernel, [VMEM] * 2, HALVES, [], 12)(filt, flat)

    def prepare(turned, after):
        kernel = functools.partial(prepare_kernel, turned)
        wide = [pltpu.VMEM((256, 256), F32)]
        (out,) = call(kernel, [VMEM, ANY], (((5, 2 * PAD, 256), BF16),), wide, 12)(band_roots, after)
        return out

    def half(matrix, hi, lo, first):
        side, far = call(side_kernel, [VMEM] * 4, (MESSAGE, FAR), [], 12)(hi, lo, w0, w)
        (mate,) = call(mate_kernel, [VMEM] * 4 + [ANY], (MESSAGE,), [], 12)(hi, lo, w0, w, side)
        side, mate, far = swap(side, 1), swap(mate, 0), pass_up(far)
        *edges, c3, c3up = call(own_kernel, [VMEM] * 4, EDGES + (COARSEST, COARSEST), [], 12)(hi, lo, w0, w)
        side, c3up = lax.optimization_barrier((side, c3up))
        passed = swap(side[TAIL:], 0)
        *edges, mate_out, side_out = call(
            vertical_kernel, [VMEM] * 8, EDGES + (MESSAGE, MESSAGE), [], 12
        )(matrix, filt, *edges, mate, side)
        y3, mate, side = call(coarse_kernel, [VMEM] * 9, (COARSEST, MESSAGE, MESSAGE), [], 12)(
            matrix, c3, c3up, far, mate, side, passed, mate_out, side_out
        )
        side, mate = swap(side, 1), swap(mate, 0)
        y0c, y1c = call(inner_kernel, [VMEM] * 5 + [ANY], INNER, [], 12)(hi, lo, w0, w, matrix, y3)
        turned = prepare(True, y3) if first else None
        (own,) = call(spread_kernel, [VMEM] * 10, (OWN_WIDE,), [], 12)(w0, w, ww, y0c, y1c, *edges, y3)
        if first:
            side, own, turned = lax.optimization_barrier((side, own, turned))
        else:
            side, own = lax.optimization_barrier((side, own))
        passed = swap(side[END_TILE:], 0)
        (got,) = call(received_kernel, [VMEM] * 5, (GOT_WIDE,), [], 12)(w0, w, ww, mate, side)
        return filt, w, ww, own, got, side, passed, turned

    *ready, turned = half(prepare(False, hi), hi, lo, True)
    hi, lo = call(middle_kernel, [VMEM] * 7, HALVES, [FAR_WIDE], 12)(*ready)
    *ready, _ = half(turned, hi, lo, False)
    (out,) = call(
        last_kernel, [VMEM] * 7, (((levels * rows, columns), F32),),
        [FAR_WIDE, pltpu.VMEM((levels * rows, columns), F32), pltpu.SemaphoreType.DMA((9,))], 12, HBM,
    )(*ready)
    return out.reshape(levels, rows, columns)


def solution(mesh):
    placed = (P("member", "lat", None), P(), P())
    return jax.shard_map(
        on_device, mesh=mesh, in_specs=placed, out_specs=P("member", "lat", None), check_vma=False
    )
```

```python
import functools
import math

import jax
import jax.numpy as jnp
from jax import lax
from jax.experimental import pallas as pl
from jax.experimental.pallas import tpu as pltpu
from jax.sharding import PartitionSpec as P


LEVELS = 4
TAPS = 5
ROOT_TWO = math.sqrt(2.0)
F32 = jnp.float32
BF16 = jnp.bfloat16
MIB = 1024 * 1024

ROWS = 16
OWN = (8, 4, 2, 1)
FIRST = -1
LAST = (8, 5, 3, 2)
BASE = (0, 10, 17, 22)
SLOTS = 26
LANES = 128
PAD = 144
KPAD = 256


def dot(a, b):
    return lax.dot_general(a, b, (((1,), (0,)), ((), ())), preferred_element_type=F32)


def dot_t(a, b):
    return lax.dot_general(a, b, (((1,), (1,)), ((), ())), preferred_element_type=F32)


def split(values):
    high = values.astype(BF16)
    return high, (values - high.astype(F32)).astype(BF16)


def slot(level, index):
    return BASE[level] + index - FIRST


def lane_ids(rows):
    return lax.broadcasted_iota(jnp.int32, (rows, LANES), 1)


def write_filters(taps_ref, filt_ref):
    signs = (1.0, -1.0, 1.0, -1.0, 1.0)
    ones = jnp.full((1, LANES), 1.0, F32)
    for level in range(LEVELS):
        for way in range(2):
            low = [taps_ref[level, way, 0, k].astype(F32) * ones for k in range(TAPS)]
            high = [taps_ref[level, way, 1, k].astype(F32) * ones for k in range(TAPS)]
            low_scale = ROOT_TWO / functools.reduce(jnp.add, low)
            high_scale = 1.0 / jnp.sqrt(functools.reduce(jnp.add, [h * h for h in high]))
            row = (level * 2 + way) * 2 * TAPS
            for k in range(TAPS):
                filt_ref[row + k : row + k + 1, :] = low[k] * low_scale
                filt_ref[row + TAPS + k : row + TAPS + k + 1, :] = (signs[k] * high[k]) * high_scale


def coeffs(filt_ref, level, way, kind):
    row = ((level * 2 + way) * 2 + kind) * TAPS
    return [filt_ref[row + k : row + k + 1, :] for k in range(TAPS)]


def product(a, b):
    a_high, a_low = split(a)
    b_high, b_low = split(b)
    return dot(a_high, b_high) + dot(a_low, b_high) + dot(a_high, b_low)


def write_weights(filt_ref, w0_ref, w_ref, ww_ref):
    row = lax.broadcasted_iota(jnp.int32, (LANES, LANES), 0)
    lane = lax.broadcasted_iota(jnp.int32, (LANES, LANES), 1)
    steps = []
    for level in range(LEVELS):
        half = (LANES // 2) >> level
        low = coeffs(filt_ref, level, 1, 0)
        high = coeffs(filt_ref, level, 1, 1)
        is_low = lane < half
        tap = row - 2 * jnp.where(is_low, lane, lane - half) + 2
        inside = (lane < 2 * half) & (row < 2 * half)
        step = jnp.zeros((LANES, LANES), F32)
        for k in range(TAPS):
            chosen = jnp.where(is_low[0:1], low[k], high[k])
            step = jnp.where(tap == k, chosen, step)
        steps.append(jnp.where(inside, step, 0.0))
    second = product(steps[0], steps[1])
    composed_steps = [steps[0], second, product(second, steps[2]), product(second, product(steps[2], steps[3]))]
    zeros = jnp.zeros((LANES, LANES), BF16)
    for level, composed in enumerate(composed_steps):
        half = (LANES // 2) >> level
        if level == 0:
            d_high, d_low = split(composed)
            moved = jnp.where(lane < half, pltpu.roll(composed, LANES - half, 1), 0.0)
            a_high, a_low = split(moved)
            w0_ref[0:LANES, 0:128] = zeros
            w0_ref[0:LANES, 128:256] = a_high
            w0_ref[0:LANES, 256:384] = zeros
            w0_ref[0:LANES, 384:512] = a_low
            w0_ref[LANES:256, 0:128] = d_high
            w0_ref[LANES:256, 128:256] = zeros
            w0_ref[LANES:256, 256:384] = d_low
            w0_ref[LANES:256, 384:512] = zeros
        else:
            moved = jnp.where((lane >= 2 * half) & (lane < 3 * half), pltpu.roll(composed, half, 1), 0.0)
            if level == LEVELS - 1:
                moved = moved + jnp.where(
                    (lane >= 3 * half) & (lane < 4 * half), pltpu.roll(composed, 3 * half, 1), 0.0
                )
            for which, values in ((0, moved), (1, composed)):
                rows = slice(which * LANES, which * LANES + LANES)
                v_high, v_low = split(values)
                w_ref[level - 1, rows, 0:128] = v_high
                w_ref[level - 1, rows, 128:256] = v_low
                ww_ref[level - 1, rows, 0:128] = v_high
                ww_ref[level - 1, rows, 128:256] = v_high


def edge_flags():
    place = lax.axis_index("lat")
    count = lax.axis_size("lat")
    lower = jnp.where(place == 0, 0.0, 1.0).astype(F32)
    upper = jnp.where(place == count - 1, 0.0, 1.0).astype(F32)
    return lower, upper


def masked(values, index, own, flags):
    if index < 0:
        return values * flags[0]
    if index >= own:
        return values * flags[1]
    return values


def latitude_analysis(rows, filt_ref, flags):
    out = {}
    for level in range(LEVELS):
        low = coeffs(filt_ref, level, 0, 0)
        high = coeffs(filt_ref, level, 0, 1)
        smooth = {}
        for index in range(FIRST, LAST[level] + 1):
            a = d = None
            for k in range(TAPS):
                source = rows.get(2 * index - 2 + k)
                if source is None:
                    continue
                a = low[k] * source if a is None else a + low[k] * source
                d = high[k] * source if d is None else d + high[k] * source
            if level < LEVELS - 1:
                a = masked(a, index, OWN[level], flags)
            smooth[index] = a
            out[slot(level, index)] = (a, d)
        rows = smooth
    return out


SPAN = ((0, ROWS - 1), (FIRST, LAST[0]), (FIRST, LAST[1]), (FIRST, LAST[2]))
SUM_BASE = (0, 16, 26, 33)
SUMS = 38


def add_term(total, term):
    return term if total is None else total + term


def own_sums(pick, filt_ref):
    out = {}
    for level in range(LEVELS):
        low = coeffs(filt_ref, level, 0, 0)
        high = coeffs(filt_ref, level, 0, 1)
        wide = {i: pick(slot(level, i)) for i in range(OWN[level])}
        first, last = SPAN[level]
        for r in range(first, last + 1):
            total = None
            for index, (a, d) in wide.items():
                k = r - 2 * index + 2
                if 0 <= k < TAPS:
                    total = add_term(total, low[k] * a + high[k] * d)
            if total is not None:
                out[SUM_BASE[level] + r - first] = total
    return out


def has_own(level, r):
    return any(0 <= r - 2 * index + 2 < TAPS for index in range(OWN[level]))


def latitude_synthesis(pick, sums, filt_ref, flags):
    rows = None
    for level in reversed(range(LEVELS)):
        low = coeffs(filt_ref, level, 0, 0)
        high = coeffs(filt_ref, level, 0, 1)
        first, last = SPAN[level]
        smooth, sharp = {}, {}
        for index in range(FIRST, LAST[level] + 1):
            if rows is not None:
                smooth[index] = rows[index]
            if not 0 <= index < OWN[level]:
                a, sharp[index] = pick(slot(level, index))
                smooth[index] = add_term(smooth.get(index), a)
        out = {}
        for r in range(first, last + 1):
            total = sums(SUM_BASE[level] + r - first) if has_own(level, r) else None
            for index in range(FIRST, LAST[level] + 1):
                k = r - 2 * index + 2
                if 0 <= k < TAPS:
                    if index in smooth:
                        total = add_term(total, low[k] * smooth[index])
                    if index in sharp:
                        total = add_term(total, high[k] * sharp[index])
            out[r] = masked(total, r, OWN[level - 1], flags) if level else total
        rows = out
    return rows


def pack(c0, c1, c2, c3, c1b, c2b, c3b=None):
    lane = lane_ids(PAD)
    last = jnp.where(lane < 64, c1b, pltpu.roll(c2b, 96, 1))
    if c3b is not None:
        last = with_far(last, c3b)
    return [
        c0[:, 0:128],
        jnp.where(lane < 64, c0[:, 128:256], jnp.where(lane < 112, pltpu.roll(c2, 64, 1), pltpu.roll(c2b, 80, 1))),
        jnp.where(lane < 96, c1, pltpu.roll(c3, 96, 1)),
        last,
    ]


def with_far(tile, c3b):
    lane = lane_ids(PAD)
    return jnp.where((lane >= 64) & (lane < 96), pltpu.roll(c3b, 64, 1), tile)


def far_of(tile):
    return pltpu.roll(tile, 64, 1)


def unpack(tiles):
    parts = [
        jnp.concatenate([tiles[0], tiles[1]], axis=1),
        tiles[2],
        pltpu.roll(tiles[1], 64, 1),
        pltpu.roll(tiles[2], 32, 1),
    ]
    if len(tiles) > 3:
        lane = lane_ids(PAD)
        parts += [tiles[3], jnp.where(lane < 32, pltpu.roll(tiles[3], 32, 1), pltpu.roll(tiles[1], 48, 1))]
    return parts


def three_bands(tile, filt_ref):
    low, high = coeffs(filt_ref, 1, 0, 0)[0], coeffs(filt_ref, 1, 0, 1)[0]
    return jnp.where(lane_ids(PAD) < 64, high * tile, pltpu.roll(low * tile, 32, 1))


def two_sums(values, filt_ref):
    ratio = coeffs(filt_ref, 1, 0, 1)[0] / coeffs(filt_ref, 1, 0, 0)[0]
    return jnp.where(lane_ids(PAD) < 32, values, pltpu.roll(values, 96, 1) + ratio * values)


def bands_of_sums(tile):
    lane = lane_ids(PAD)
    return jnp.where(lane < 32, tile, jnp.where(lane < 64, 0.0, pltpu.roll(tile, 32, 1)))


def pack_coarse(c3):
    lane = lane_ids(40)
    last = jnp.concatenate([c3[120:144], jnp.zeros((16, LANES), F32)], axis=0)
    return jnp.where(
        lane < 32,
        c3[0:40],
        jnp.where(
            lane < 64,
            pltpu.roll(c3[40:80], 32, 1),
            jnp.where(lane < 96, pltpu.roll(c3[80:120], 64, 1), pltpu.roll(last, 96, 1)),
        ),
    )


def unpack_coarse(values):
    parts = [values] + [pltpu.roll(values, LANES - 32 * q, 1) for q in (1, 2, 3)]
    return jnp.concatenate(parts[:3] + [parts[3][0:24]], axis=0)


def is_even():
    return lax.rem(lax.axis_index("lat"), 2) == 0


MAIN = 136
ORDERED = (0, 1, 3, 2)
ENDS = 4 * MAIN
TAIL = 2 * MAIN
END_TILE = 3 * MAIN


def join(main, end):
    top = lax.broadcasted_iota(jnp.int32, (8, LANES), 0) == 0
    return jnp.concatenate([main, jnp.where(top, end, 0.0)], axis=0)


def part(ref, t, start=0):
    at = ORDERED[t] * MAIN - start
    end = ENDS + t - start
    return join(ref[at : at + MAIN, :], ref[end : end + 1, :])


def put_one(ref, t, tile):
    ref[ORDERED[t] * MAIN : ORDERED[t] * MAIN + MAIN, :] = tile[0:MAIN]
    ref[ENDS + t : ENDS + t + 1, :] = tile[MAIN : MAIN + 1]


def put(ref, tiles):
    ref[ENDS : ENDS + 8, :] = jnp.zeros((8, LANES), F32)
    for t, tile in enumerate(tiles):
        put_one(ref, t, tile)


def received(mate_ref, side_ref, n_below, n_above):
    even = is_even()
    place = lax.axis_index("lat")
    no_below = place == 0
    no_above = place == lax.axis_size("lat") - 1
    below, above = [], []
    for t in range(max(n_below, n_above)):
        mate, side = part(mate_ref, t), part(side_ref, t)
        if t < n_below:
            below.append(jnp.where(no_below, 0.0, jnp.where(even, side, mate)))
        if t < n_above:
            above.append(jnp.where(no_above, 0.0, jnp.where(even, mate, side)))
    return below, above


def store_split(hi_ref, lo_ref, out, at):
    for place, (a, d) in out.items():
        for part, values in ((0, a), (1, d)):
            lanes = slice(part * LANES, part * LANES + LANES)
            high, low = split(values)
            hi_ref[place, at, lanes] = high
            lo_ref[place, at, lanes] = low


def stack(parts):
    return jnp.concatenate(parts, axis=0)


def bands(hi_ref, lo_ref, w0_ref, w_ref):
    def level0(*slots):
        w_high, w_low = w0_ref[:, 0:256], w0_ref[:, 256:512]
        high, low = stack([hi_ref[s] for s in slots]), stack([lo_ref[s] for s in slots])
        out = dot(high, w_high) + dot(high, w_low) + dot(low, w_high)
        return [out[i * PAD : i * PAD + PAD] for i in range(len(slots))]

    def others(level, *slots):
        high, low = stack([hi_ref[s] for s in slots]), stack([lo_ref[s] for s in slots])
        both = dot(high, w_ref[level - 1])
        out = both[:, 0:128] + both[:, 128:256] + dot(low, w_ref[level - 1, :, 0:128])
        return [out[i * PAD : i * PAD + PAD] for i in range(len(slots))]

    return level0, others


def sums_message(hi_ref, lo_ref, w0_ref, w_ref, upward, extra):
    level0, others = bands(hi_ref, lo_ref, w0_ref, w_ref)

    def chosen(level, up_index):
        return jnp.where(upward, slot(level, up_index), slot(level, -1))

    (c0,) = level0(chosen(0, 8))
    (c1,) = others(1, chosen(1, 4))
    row = slot(0, 8)
    both = dot(hi_ref[row, :, 0:128], w_ref[0, 128:256, :])
    c1b = both[:, 0:128] + both[:, 128:256] + dot(lo_ref[row, :, 0:128], w_ref[0, 128:256, 0:128])
    c2, c2b = others(2, chosen(2, 2), slot(2, 3))
    c3, more = others(3, chosen(3, 1), slot(3, extra))
    return pack(c0, c1, c2, c3, c1b, c2b, more), more


def apply_vertical(m_ref, band, values):
    high, low = split(values)
    zeros = jnp.zeros((KPAD - PAD, values.shape[1]), BF16)
    high = jnp.concatenate([high, zeros], axis=0)
    low = jnp.concatenate([low, zeros], axis=0)
    both = dot(m_ref[band], high)
    return both[0:PAD] + both[PAD:] + dot(m_ref[band, 0:PAD], low)


def spread_level0(values, w0_ref):
    high, low = split(stack(values))
    w_high, w_low = w0_ref[:, 0:256], w0_ref[:, 256:512]
    out = dot_t(high, w_high) + dot_t(low, w_high) + dot_t(high, w_low)
    return [out[i * PAD : i * PAD + PAD] for i in range(len(values))]


def spread_other(level, values, w_ref, ww_ref):
    high, low = split(stack(values))
    pair = jnp.concatenate([high, low], axis=1)
    out = dot_t(pair, ww_ref[level - 1]) + dot_t(high, w_ref[level - 1, :, 128:256])
    return [out[i * PAD : i * PAD + PAD] for i in range(len(values))]


OWN_BASE = (0, 8, 12, 14)
GOT = {(0, -1): 0, (0, 8): 1, (1, -1): 2, (1, 4): 3, (1, 5): 4, (2, -1): 5, (2, 2): 6, (2, 3): 7, (3, -1): 8, (3, 1): 9}


def pick_at(got_ref, far_ref, at):
    table = {slot(level, index): (got_ref, place) for (level, index), place in GOT.items()}
    table[slot(3, 2)] = (far_ref, 0)

    def pick(place):
        ref, i = table[place]
        return ref[i, at, 0:128], ref[i, at, 128:256]

    return pick


def own_at(own_ref, at):
    def pick(place):
        level = max(i for i in range(LEVELS) if BASE[i] <= place)
        i = OWN_BASE[level] + place - slot(level, 0)
        return own_ref[i, at, 0:128], own_ref[i, at, 128:256]

    return pick


def weights_kernel(taps_ref, filt_ref, w0_ref, w_ref, ww_ref):
    write_filters(taps_ref, filt_ref)
    write_weights(filt_ref, w0_ref, w_ref, ww_ref)


def first_kernel(filt_ref, x_ref, hi_ref, lo_ref):
    flags = edge_flags()

    def chunk(c, carry):
        start = pl.multiple_of(c * (16 * ROWS), 16 * ROWS)
        rows = {r: x_ref[pl.ds(start + r, 16, stride=ROWS), :] for r in range(ROWS)}
        at = pl.ds(pl.multiple_of(c * 16, 16), 16)
        store_split(hi_ref, lo_ref, latitude_analysis(rows, filt_ref, flags), at)
        return carry

    lax.fori_loop(0, 8, chunk, 0)
    top = lax.broadcasted_iota(jnp.int32, (8, LANES), 0) == 0
    rows = {}
    for r in range(ROWS):
        head = x_ref[pl.ds(128 * ROWS + r, 8, stride=ROWS), :]
        tail = jnp.where(top, x_ref[136 * ROWS + r : 136 * ROWS + r + 1, :], 0.0)
        rows[r] = jnp.concatenate([head, tail], axis=0)
    store_split(hi_ref, lo_ref, latitude_analysis(rows, filt_ref, flags), slice(128, 144))


def side_kernel(hi_ref, lo_ref, w0_ref, w_ref, side_ref, far_ref):
    tiles, share = sums_message(hi_ref, lo_ref, w0_ref, w_ref, jnp.logical_not(is_even()), 2)
    put(side_ref, tiles)
    far_ref[...] = pack_coarse(share)


def mate_kernel(hi_ref, lo_ref, w0_ref, w_ref, after_ref, mate_ref):
    del after_ref
    tiles, _ = sums_message(hi_ref, lo_ref, w0_ref, w_ref, is_even(), 0)
    put(mate_ref, tiles)


def own_kernel(hi_ref, lo_ref, w0_ref, w_ref, c0_ref, c1_ref, c1b_ref, c2_ref, c3_ref, c3up_ref):
    level0, others = bands(hi_ref, lo_ref, w0_ref, w_ref)
    c0_ref[0], c0_ref[1] = level0(slot(0, 0), slot(0, 7))
    c1_ref[:, 0:128], c1_ref[:, 128:256], c1b_ref[...] = others(1, slot(1, 0), slot(1, 1), slot(1, 3))
    c2_ref[:, 0:128], c2_ref[:, 128:256] = others(2, slot(2, 0), slot(2, 1))
    c3_ref[...], c3up_ref[...] = others(3, slot(3, 0), slot(3, 1))


def inner_kernel(hi_ref, lo_ref, w0_ref, w_ref, m_ref, after_ref, y0_ref, y1_ref):
    del after_ref
    level0, others = bands(hi_ref, lo_ref, w0_ref, w_ref)
    y1_ref[...] = apply_vertical(m_ref, 1, others(1, slot(1, 2))[0])
    for i, c0 in enumerate(level0(*[slot(0, i) for i in range(1, 7)])):
        y0_ref[i] = apply_vertical(m_ref, 0, c0)


def vertical_kernel(m_ref, filt_ref, c0_ref, c1_ref, c1b_ref, c2_ref, mate_ref, side_ref,
                    y0_ref, y1_ref, y1b_ref, y2_ref, mate_out_ref, side_out_ref):
    below, above = received(mate_ref, side_ref, 4, 3)
    below, above = unpack(below), unpack(above)
    c2 = c2_ref[...]
    y2 = apply_vertical(m_ref, 2, jnp.concatenate([c2[:, 0:128] + below[2], c2[:, 128:256] + below[5] + above[2]], axis=1))
    c1 = c1_ref[...]
    y1 = apply_vertical(m_ref, 1, jnp.concatenate([c1[:, 0:128] + below[1], c1[:, 128:256] + three_bands(below[4], filt_ref)], axis=1))
    y1b = apply_vertical(m_ref, 1, c1b_ref[...] + above[1])
    first = apply_vertical(m_ref, 0, c0_ref[0] + below[0])
    last = apply_vertical(m_ref, 0, c0_ref[1] + above[0])
    y0_ref[0] = first
    y0_ref[1] = last
    y1_ref[...] = y1
    y1b_ref[...] = y1b
    y2_ref[...] = y2
    none = jnp.zeros((PAD, LANES), F32)
    sums = two_sums(y1[:, 128:256], filt_ref)
    down = pack(first, y1[:, 0:128], y2[:, 0:128], none, sums, y2[:, 128:256])
    up = pack(last, y1b, y2[:, 128:256], none, sums, y2[:, 128:256])
    even = is_even()
    put(side_out_ref, [jnp.where(even, d, u) for d, u in zip(down, up)])
    put(mate_out_ref, [jnp.where(even, u, d) for d, u in zip(down, up)])


def coarse_kernel(m_ref, c3_ref, c3up_ref, far_ref, mate_ref, side_ref, passed_ref, mate_in_ref, side_in_ref,
                  y3_ref, mate_out_ref, side_out_ref):
    even = is_even()
    place = lax.axis_index("lat")
    last = lax.axis_size("lat") - 1
    lane = lane_ids(PAD)
    from_side = jnp.where((place == 0) | (place == last), 0.0, pltpu.roll(part(side_ref, 2), 32, 1))
    passed = far_of(part(passed_ref, 3, TAIL))
    passed = jnp.where(even, unpack_coarse(far_ref[...]), jnp.where(place == 1, 0.0, passed))
    mine = c3_ref[...] + pltpu.roll(part(mate_ref, 2), 32, 1) + from_side + passed
    coarse = jnp.where(place == 0, 0.0, far_of(part(side_ref, 3)))
    above = jnp.where(place == last - 1, 0.0, pltpu.roll(part(passed_ref, 2, TAIL), 32, 1))
    other = far_of(part(mate_ref, 3)) + c3up_ref[...] + coarse + above
    both = jnp.concatenate([mine, other], axis=1)
    detail, smooth = apply_vertical(m_ref, 3, both), apply_vertical(m_ref, 4, both)
    y3 = jnp.where(lane < 24, detail[:, 0:128], smooth[:, 0:128])
    y3_ref[...] = y3
    moved = pltpu.roll(y3, 96, 1)
    mate_out_ref[...] = mate_in_ref[...]
    put_one(mate_out_ref, 2, jnp.where(lane < 96, part(mate_in_ref, 2), moved))
    side_out_ref[...] = side_in_ref[...]
    put_one(side_out_ref, 2, jnp.where(lane < 96, part(side_in_ref, 2), moved))
    y3_other = jnp.where(lane < 24, detail[:, 128:256], smooth[:, 128:256])
    put_one(side_out_ref, 3, with_far(part(side_in_ref, 3), y3_other))


def spread_kernel(filt_ref, w0_ref, w_ref, ww_ref, y0c_ref, y1c_ref, y0_ref, y1_ref, y1b_ref, y2_ref, y3_ref, sums_ref,
                  own_ref):
    level0 = [y0_ref[i // 7] if i in (0, 7) else y0c_ref[i - 1] for i in range(8)]
    level1 = [y1_ref[:, 0:128], y1_ref[:, 128:256], y1c_ref[...], y1b_ref[...]]
    level2 = [y2_ref[:, 0:128], y2_ref[:, 128:256]]
    wide = spread_level0(level0, w0_ref)
    for level, values in ((1, level1), (2, level2), (3, [y3_ref[...]])):
        wide += spread_other(level, values, w_ref, ww_ref)
    for i, values in enumerate(wide):
        own_ref[i] = values

    def chunk(c, carry):
        at = pl.ds(pl.multiple_of(c * 16, 16), 16)
        for place, total in own_sums(own_at(own_ref, at), filt_ref).items():
            sums_ref[place, at, :] = total
        return carry

    lax.fori_loop(0, 9, chunk, 0)


def received_kernel(w0_ref, w_ref, ww_ref, mate_ref, side_ref, got_ref):
    below, above = received(mate_ref, side_ref, 3, 4)
    below, above = unpack(below), unpack(above)
    wide = spread_level0([below[0], above[0]], w0_ref)
    wide += spread_other(1, [below[1], above[1], bands_of_sums(above[4])], w_ref, ww_ref)
    wide += spread_other(2, [below[2], above[2], above[5]], w_ref, ww_ref)
    wide += spread_other(3, [below[3], above[3]], w_ref, ww_ref)
    for i, values in enumerate(wide):
        got_ref[i] = values


def spread_coarse(side_ref, passed_ref, w_ref, ww_ref, far_ref):
    value = jnp.where(is_even(), pltpu.roll(part(passed_ref, 2, END_TILE), 32, 1), far_of(part(side_ref, 3)))
    value = jnp.where(lax.axis_index("lat") >= lax.axis_size("lat") - 2, 0.0, value)
    far_ref[0] = spread_other(3, [value], w_ref, ww_ref)[0]


def middle_kernel(filt_ref, w_ref, ww_ref, sums_ref, got_ref, side_ref, passed_ref, hi_ref, lo_ref, far_ref):
    flags = edge_flags()
    spread_coarse(side_ref, passed_ref, w_ref, ww_ref, far_ref)

    def chunk(c, carry):
        at = pl.ds(pl.multiple_of(c * 16, 16), 16)
        rows = latitude_synthesis(pick_at(got_ref, far_ref, at), lambda i: sums_ref[i, at, :], filt_ref, flags)
        store_split(hi_ref, lo_ref, latitude_analysis(rows, filt_ref, flags), at)
        return carry

    lax.fori_loop(0, 9, chunk, 0)


def last_kernel(filt_ref, w_ref, ww_ref, sums_ref, got_ref, side_ref, passed_ref, out_hbm, far_ref, out_ref, sems):
    flags = edge_flags()
    spread_coarse(side_ref, passed_ref, w_ref, ww_ref, far_ref)

    def leave(c):
        piece = pl.ds(pl.multiple_of(c * (16 * ROWS), 16 * ROWS), 16 * ROWS)
        return pltpu.make_async_copy(out_ref.at[piece, :], out_hbm.at[piece, :], sems.at[c])

    def chunk(c, carry):
        at = pl.ds(pl.multiple_of(c * 16, 16), 16)
        rows = latitude_synthesis(pick_at(got_ref, far_ref, at), lambda i: sums_ref[i, at, :], filt_ref, flags)
        start = pl.multiple_of(c * (16 * ROWS), 16 * ROWS)
        for r, values in rows.items():
            out_ref[pl.ds(start + r, 16, stride=ROWS), :] = values
        leave(c).start()
        return carry

    lax.fori_loop(0, 8, chunk, 0)
    end = slice(128, 144)
    rows = latitude_synthesis(pick_at(got_ref, far_ref, end), lambda i: sums_ref[i, end, :], filt_ref, flags)
    for r, values in rows.items():
        out_ref[pl.ds(128 * ROWS + r, 8, stride=ROWS), :] = values[0:8]
        out_ref[136 * ROWS + r : 136 * ROWS + r + 1, :] = values[8:9]
    rest = pl.ds(128 * ROWS, 9 * ROWS)
    tail = pltpu.make_async_copy(out_ref.at[rest, :], out_hbm.at[rest, :], sems.at[8])
    tail.start()
    for c in range(8):
        leave(c).wait()
    tail.wait()


def prepare_kernel(turned, m_ref, after_ref, out_ref, wide_ref):
    del after_ref
    levels = m_ref.shape[1]
    wide_ref[...] = jnp.zeros_like(wide_ref)
    for band in range(m_ref.shape[0]):
        wide_ref[0:levels, 0:levels] = m_ref[band]
        matrix = wide_ref[...].T if turned else wide_ref[...]
        high, low = split(matrix[0:PAD])
        out_ref[band, 0:PAD, :] = high
        out_ref[band, PAD : 2 * PAD, :] = low


VMEM = pl.BlockSpec(memory_space=pltpu.VMEM)
SMEM = pl.BlockSpec(memory_space=pltpu.SMEM)
HBM = pl.BlockSpec(memory_space=pltpu.HBM)
ANY = pl.BlockSpec(memory_space=pl.ANY)

MESSAGE = ((4 * MAIN + 8, LANES), F32)
FAR = ((40, LANES), F32)
WEIGHTS = (((80, LANES), F32), ((256, 512), BF16), ((3, 256, 256), BF16), ((3, 256, 256), BF16))
HALVES = (((SLOTS, PAD, 256), BF16),) * 2
EDGES = (((2, PAD, 256), F32), ((PAD, 256), F32), ((PAD, LANES), F32), ((PAD, 256), F32))
COARSEST = ((PAD, LANES), F32)
INNER = (((6, PAD, 256), F32), ((PAD, LANES), F32))
OWN_SUMS = ((SUMS, PAD, LANES), F32)
OWN_WIDE = pltpu.VMEM((15, PAD, 256), F32)
GOT_WIDE = ((10, PAD, 256), F32)
FAR_WIDE = pltpu.VMEM((1, PAD, 256), F32)


def call(kernel, in_specs, outs, scratch, limit, out_spec=VMEM):
    return pl.pallas_call(
        kernel,
        out_shape=[jax.ShapeDtypeStruct(shape, dtype) for shape, dtype in outs],
        in_specs=in_specs,
        out_specs=[out_spec] * len(outs),
        scratch_shapes=scratch,
        compiler_params=pltpu.CompilerParams(vmem_limit_bytes=limit * MIB),
        cost_estimate=pl.CostEstimate(flops=10**9, bytes_accessed=8 * MIB, transcendentals=0),
    )


def swap(values, phase):
    count = lax.axis_size("lat")
    partner = {}
    for i in range(phase, count - 1, 2):
        partner[i], partner[i + 1] = i + 1, i
    return lax.ppermute(values, "lat", [(i, partner.get(i, i)) for i in range(count)])


def pass_up(values):
    count = lax.axis_size("lat")
    return lax.ppermute(values, "lat", [(i, i + 2) for i in range(0, count - 2, 2)])


def on_device(increment, filter_taps, band_roots):
    levels, rows, columns = increment.shape
    flat = increment.reshape(levels * rows, columns)
    filt, w0, w, ww = call(weights_kernel, [SMEM], WEIGHTS, [], 12)(filter_taps)
    hi, lo = call(first_kernel, [VMEM] * 2, HALVES, [], 12)(filt, flat)

    def prepare(turned, after):
        kernel = functools.partial(prepare_kernel, turned)
        wide = [pltpu.VMEM((256, 256), F32)]
        (out,) = call(kernel, [VMEM, ANY], (((5, 2 * PAD, 256), BF16),), wide, 12)(band_roots, after)
        return out

    def half(transposed, hi, lo):
        side, far = call(side_kernel, [VMEM] * 4, (MESSAGE, FAR), [], 12)(hi, lo, w0, w)
        (mate,) = call(mate_kernel, [VMEM] * 4 + [ANY], (MESSAGE,), [], 12)(hi, lo, w0, w, side)
        side, mate, far = swap(side, 1), swap(mate, 0), pass_up(far)
        *edges, c3, c3up = call(own_kernel, [VMEM] * 4, EDGES + (COARSEST, COARSEST), [], 12)(hi, lo, w0, w)
        matrix = prepare(transposed, c3up)
        side, matrix = lax.optimization_barrier((side, matrix))
        passed = swap(side[TAIL:], 0)
        *edges, mate_out, side_out = call(
            vertical_kernel, [VMEM] * 8, EDGES + (MESSAGE, MESSAGE), [], 12
        )(matrix, filt, *edges, mate, side)
        y3, mate, side = call(coarse_kernel, [VMEM] * 9, (COARSEST, MESSAGE, MESSAGE), [], 12)(
            matrix, c3, c3up, far, mate, side, passed, mate_out, side_out
        )
        side, mate = swap(side, 1), swap(mate, 0)
        y0c, y1c = call(inner_kernel, [VMEM] * 5 + [ANY], INNER, [], 12)(hi, lo, w0, w, matrix, y3)
        (own,) = call(spread_kernel, [VMEM] * 11, (OWN_SUMS,), [OWN_WIDE], 12)(filt, w0, w, ww, y0c, y1c, *edges, y3)
        side, own = lax.optimization_barrier((side, own))
        passed = swap(side[END_TILE:], 0)
        (got,) = call(received_kernel, [VMEM] * 5, (GOT_WIDE,), [], 12)(w0, w, ww, mate, side)
        return filt, w, ww, own, got, side, passed

    ready = half(False, hi, lo)
    hi, lo = call(middle_kernel, [VMEM] * 7, HALVES, [FAR_WIDE], 12)(*ready)
    ready = half(True, hi, lo)
    (out,) = call(
        last_kernel, [VMEM] * 7, (((levels * rows, columns), F32),),
        [FAR_WIDE, pltpu.VMEM((levels * rows, columns), F32), pltpu.SemaphoreType.DMA((9,))], 12, HBM,
    )(*ready)
    return out.reshape(levels, rows, columns)


def solution(mesh):
    placed = (P("member", "lat", None), P(), P())
    return jax.shard_map(
        on_device, mesh=mesh, in_specs=placed, out_specs=P("member", "lat", None), check_vma=False
    )
```

```python
import functools
import math

import jax
import jax.numpy as jnp
from jax import lax
from jax.experimental import pallas as pl
from jax.experimental.pallas import tpu as pltpu
from jax.sharding import PartitionSpec as P


LEVELS = 4
TAPS = 5
ROOT_TWO = math.sqrt(2.0)
F32 = jnp.float32
BF16 = jnp.bfloat16
MIB = 1024 * 1024

ROWS = 16
OWN = (8, 4, 2, 1)
FIRST = -1
LAST = (8, 5, 3, 2)
BASE = (0, 10, 17, 22)
SLOTS = 26
LANES = 128
PAD = 144
KPAD = 256


def dot(a, b):
    return lax.dot_general(a, b, (((1,), (0,)), ((), ())), preferred_element_type=F32)


def dot_t(a, b):
    return lax.dot_general(a, b, (((1,), (1,)), ((), ())), preferred_element_type=F32)


def split(values):
    high = values.astype(BF16)
    return high, (values - high.astype(F32)).astype(BF16)


def slot(level, index):
    return BASE[level] + index - FIRST


def lane_ids(rows):
    return lax.broadcasted_iota(jnp.int32, (rows, LANES), 1)


def write_filters(taps_ref, filt_ref):
    signs = (1.0, -1.0, 1.0, -1.0, 1.0)
    ones = jnp.full((1, LANES), 1.0, F32)
    for level in range(LEVELS):
        for way in range(2):
            low = [taps_ref[level, way, 0, k].astype(F32) * ones for k in range(TAPS)]
            high = [taps_ref[level, way, 1, k].astype(F32) * ones for k in range(TAPS)]
            low_scale = ROOT_TWO / functools.reduce(jnp.add, low)
            high_scale = 1.0 / jnp.sqrt(functools.reduce(jnp.add, [h * h for h in high]))
            row = (level * 2 + way) * 2 * TAPS
            for k in range(TAPS):
                filt_ref[row + k : row + k + 1, :] = low[k] * low_scale
                filt_ref[row + TAPS + k : row + TAPS + k + 1, :] = (signs[k] * high[k]) * high_scale


def coeffs(filt_ref, level, way, kind):
    row = ((level * 2 + way) * 2 + kind) * TAPS
    return [filt_ref[row + k : row + k + 1, :] for k in range(TAPS)]


def product(a, b):
    a_high, a_low = split(a)
    b_high, b_low = split(b)
    return dot(a_high, b_high) + dot(a_low, b_high) + dot(a_high, b_low)


def write_weights(filt_ref, w0_ref, w_ref, ww_ref):
    row = lax.broadcasted_iota(jnp.int32, (LANES, LANES), 0)
    lane = lax.broadcasted_iota(jnp.int32, (LANES, LANES), 1)
    steps = []
    for level in range(LEVELS):
        half = (LANES // 2) >> level
        low = coeffs(filt_ref, level, 1, 0)
        high = coeffs(filt_ref, level, 1, 1)
        is_low = lane < half
        tap = row - 2 * jnp.where(is_low, lane, lane - half) + 2
        inside = (lane < 2 * half) & (row < 2 * half)
        step = jnp.zeros((LANES, LANES), F32)
        for k in range(TAPS):
            chosen = jnp.where(is_low[0:1], low[k], high[k])
            step = jnp.where(tap == k, chosen, step)
        steps.append(jnp.where(inside, step, 0.0))
    second = product(steps[0], steps[1])
    composed_steps = [steps[0], second, product(second, steps[2]), product(second, product(steps[2], steps[3]))]
    zeros = jnp.zeros((LANES, LANES), BF16)
    for level, composed in enumerate(composed_steps):
        half = (LANES // 2) >> level
        if level == 0:
            d_high, d_low = split(composed)
            moved = jnp.where(lane < half, pltpu.roll(composed, LANES - half, 1), 0.0)
            a_high, a_low = split(moved)
            w0_ref[0:LANES, 0:128] = zeros
            w0_ref[0:LANES, 128:256] = a_high
            w0_ref[0:LANES, 256:384] = zeros
            w0_ref[0:LANES, 384:512] = a_low
            w0_ref[LANES:256, 0:128] = d_high
            w0_ref[LANES:256, 128:256] = zeros
            w0_ref[LANES:256, 256:384] = d_low
            w0_ref[LANES:256, 384:512] = zeros
        else:
            moved = jnp.where((lane >= 2 * half) & (lane < 3 * half), pltpu.roll(composed, half, 1), 0.0)
            if level == LEVELS - 1:
                moved = moved + jnp.where(
                    (lane >= 3 * half) & (lane < 4 * half), pltpu.roll(composed, 3 * half, 1), 0.0
                )
            for which, values in ((0, moved), (1, composed)):
                rows = slice(which * LANES, which * LANES + LANES)
                v_high, v_low = split(values)
                w_ref[level - 1, rows, 0:128] = v_high
                w_ref[level - 1, rows, 128:256] = v_low
                ww_ref[level - 1, rows, 0:128] = v_high
                ww_ref[level - 1, rows, 128:256] = v_high


def edge_flags():
    place = lax.axis_index("lat")
    count = lax.axis_size("lat")
    lower = jnp.where(place == 0, 0.0, 1.0).astype(F32)
    upper = jnp.where(place == count - 1, 0.0, 1.0).astype(F32)
    return lower, upper


def masked(values, index, own, flags):
    if index < 0:
        return values * flags[0]
    if index >= own:
        return values * flags[1]
    return values


def latitude_analysis(rows, filt_ref, flags):
    out = {}
    for level in range(LEVELS):
        low = coeffs(filt_ref, level, 0, 0)
        high = coeffs(filt_ref, level, 0, 1)
        smooth = {}
        for index in range(FIRST, LAST[level] + 1):
            a = d = None
            for k in range(TAPS):
                source = rows.get(2 * index - 2 + k)
                if source is None:
                    continue
                a = low[k] * source if a is None else a + low[k] * source
                d = high[k] * source if d is None else d + high[k] * source
            if level < LEVELS - 1:
                a = masked(a, index, OWN[level], flags)
            smooth[index] = a
            out[slot(level, index)] = (a, d)
        rows = smooth
    return out


SPAN = ((0, ROWS - 1), (FIRST, LAST[0]), (FIRST, LAST[1]), (FIRST, LAST[2]))
SUM_BASE = (0, 16, 26, 33)
SUMS = 38


def add_term(total, term):
    return term if total is None else total + term


def own_sums(pick, filt_ref):
    out = {}
    for level in range(LEVELS):
        low = coeffs(filt_ref, level, 0, 0)
        high = coeffs(filt_ref, level, 0, 1)
        wide = {i: pick(slot(level, i)) for i in range(OWN[level])}
        first, last = SPAN[level]
        for r in range(first, last + 1):
            total = None
            for index, (a, d) in wide.items():
                k = r - 2 * index + 2
                if 0 <= k < TAPS:
                    total = add_term(total, low[k] * a + high[k] * d)
            if total is not None:
                out[SUM_BASE[level] + r - first] = total
    return out


def has_own(level, r):
    return any(0 <= r - 2 * index + 2 < TAPS for index in range(OWN[level]))


def latitude_synthesis(pick, sums, filt_ref, flags):
    rows = None
    for level in reversed(range(LEVELS)):
        low = coeffs(filt_ref, level, 0, 0)
        high = coeffs(filt_ref, level, 0, 1)
        first, last = SPAN[level]
        smooth, sharp = {}, {}
        for index in range(FIRST, LAST[level] + 1):
            if rows is not None:
                smooth[index] = rows[index]
            if not 0 <= index < OWN[level]:
                a, sharp[index] = pick(slot(level, index))
                smooth[index] = add_term(smooth.get(index), a)
        out = {}
        for r in range(first, last + 1):
            total = sums(SUM_BASE[level] + r - first) if has_own(level, r) else None
            for index in range(FIRST, LAST[level] + 1):
                k = r - 2 * index + 2
                if 0 <= k < TAPS:
                    if index in smooth:
                        total = add_term(total, low[k] * smooth[index])
                    if index in sharp:
                        total = add_term(total, high[k] * sharp[index])
            out[r] = masked(total, r, OWN[level - 1], flags) if level else total
        rows = out
    return rows


def pack(c0, c1, c2, c3, c1b, c2b, c3b=None):
    lane = lane_ids(PAD)
    last = jnp.where(lane < 64, c1b, pltpu.roll(c3, 96, 1))
    if c3b is not None:
        last = with_far(last, c3b)
    return [
        c0[:, 0:128],
        jnp.where(lane < 64, c0[:, 128:256], jnp.where(lane < 112, pltpu.roll(c2, 64, 1), pltpu.roll(c2b, 80, 1))),
        jnp.where(lane < 96, c1, pltpu.roll(c2b, 96, 1)),
        last,
    ]


def with_far(tile, c3b):
    lane = lane_ids(PAD)
    return jnp.where((lane >= 64) & (lane < 96), pltpu.roll(c3b, 64, 1), tile)


def far_of(tile):
    return pltpu.roll(tile, 64, 1)


def unpack(tiles):
    parts = [
        jnp.concatenate([tiles[0], tiles[1]], axis=1),
        tiles[2],
        pltpu.roll(tiles[1], 64, 1),
        pltpu.roll(tiles[3], 32, 1),
    ]
    second = jnp.where(lane_ids(PAD) < 32, pltpu.roll(tiles[2], 32, 1), pltpu.roll(tiles[1], 48, 1))
    return parts + [tiles[3], second]


def three_bands(tile, filt_ref):
    low, high = coeffs(filt_ref, 1, 0, 0)[0], coeffs(filt_ref, 1, 0, 1)[0]
    return jnp.where(lane_ids(PAD) < 64, high * tile, pltpu.roll(low * tile, 32, 1))


def two_sums(values, filt_ref):
    ratio = coeffs(filt_ref, 1, 0, 1)[0] / coeffs(filt_ref, 1, 0, 0)[0]
    return jnp.where(lane_ids(PAD) < 32, values, pltpu.roll(values, 96, 1) + ratio * values)


def bands_of_sums(tile):
    lane = lane_ids(PAD)
    return jnp.where(lane < 32, tile, jnp.where(lane < 64, 0.0, pltpu.roll(tile, 32, 1)))


def pack_coarse(c3):
    lane = lane_ids(40)
    last = jnp.concatenate([c3[120:144], jnp.zeros((16, LANES), F32)], axis=0)
    return jnp.where(
        lane < 32,
        c3[0:40],
        jnp.where(
            lane < 64,
            pltpu.roll(c3[40:80], 32, 1),
            jnp.where(lane < 96, pltpu.roll(c3[80:120], 64, 1), pltpu.roll(last, 96, 1)),
        ),
    )


def unpack_coarse(values):
    parts = [values] + [pltpu.roll(values, LANES - 32 * q, 1) for q in (1, 2, 3)]
    return jnp.concatenate(parts[:3] + [parts[3][0:24]], axis=0)


def is_even():
    return lax.rem(lax.axis_index("lat"), 2) == 0


MAIN = 136
ORDERED = (0, 1, 2, 3)
ENDS = 4 * MAIN
TAIL = 3 * MAIN


def join(main, end):
    top = lax.broadcasted_iota(jnp.int32, (8, LANES), 0) == 0
    return jnp.concatenate([main, jnp.where(top, end, 0.0)], axis=0)


def part(ref, t, start=0):
    at = ORDERED[t] * MAIN - start
    end = ENDS + t - start
    return join(ref[at : at + MAIN, :], ref[end : end + 1, :])


def put_one(ref, t, tile):
    ref[ORDERED[t] * MAIN : ORDERED[t] * MAIN + MAIN, :] = tile[0:MAIN]
    ref[ENDS + t : ENDS + t + 1, :] = tile[MAIN : MAIN + 1]


def put(ref, tiles):
    ref[ENDS : ENDS + 8, :] = jnp.zeros((8, LANES), F32)
    for t, tile in enumerate(tiles):
        put_one(ref, t, tile)


def received(mate_ref, side_ref, n_below, n_above):
    even = is_even()
    place = lax.axis_index("lat")
    no_below = place == 0
    no_above = place == lax.axis_size("lat") - 1
    below, above = [], []
    for t in range(max(n_below, n_above)):
        mate, side = part(mate_ref, t), part(side_ref, t)
        if t < n_below:
            below.append(jnp.where(no_below, 0.0, jnp.where(even, side, mate)))
        if t < n_above:
            above.append(jnp.where(no_above, 0.0, jnp.where(even, mate, side)))
    return below, above


def store_split(hi_ref, lo_ref, out, at):
    for place, (a, d) in out.items():
        for part, values in ((0, a), (1, d)):
            lanes = slice(part * LANES, part * LANES + LANES)
            high, low = split(values)
            hi_ref[place, at, lanes] = high
            lo_ref[place, at, lanes] = low


def stack(parts):
    return jnp.concatenate(parts, axis=0)


def bands(hi_ref, lo_ref, w0_ref, w_ref):
    def level0(*slots):
        w_high, w_low = w0_ref[:, 0:256], w0_ref[:, 256:512]
        high, low = stack([hi_ref[s] for s in slots]), stack([lo_ref[s] for s in slots])
        out = dot(high, w_high) + dot(high, w_low) + dot(low, w_high)
        return [out[i * PAD : i * PAD + PAD] for i in range(len(slots))]

    def others(level, *slots):
        high, low = stack([hi_ref[s] for s in slots]), stack([lo_ref[s] for s in slots])
        both = dot(high, w_ref[level - 1])
        out = both[:, 0:128] + both[:, 128:256] + dot(low, w_ref[level - 1, :, 0:128])
        return [out[i * PAD : i * PAD + PAD] for i in range(len(slots))]

    return level0, others


def sums_message(hi_ref, lo_ref, w0_ref, w_ref, upward, extra):
    level0, others = bands(hi_ref, lo_ref, w0_ref, w_ref)

    def chosen(level, up_index):
        return jnp.where(upward, slot(level, up_index), slot(level, -1))

    (c0,) = level0(chosen(0, 8))
    (c1,) = others(1, chosen(1, 4))
    row = slot(0, 8)
    both = dot(hi_ref[row, :, 0:128], w_ref[0, 128:256, :])
    c1b = both[:, 0:128] + both[:, 128:256] + dot(lo_ref[row, :, 0:128], w_ref[0, 128:256, 0:128])
    c2, c2b = others(2, chosen(2, 2), slot(2, 3))
    c3, more = others(3, chosen(3, 1), slot(3, extra))
    return pack(c0, c1, c2, c3, c1b, c2b, more), more


def apply_vertical(m_ref, band, values):
    high, low = split(values)
    zeros = jnp.zeros((KPAD - PAD, values.shape[1]), BF16)
    high = jnp.concatenate([high, zeros], axis=0)
    low = jnp.concatenate([low, zeros], axis=0)
    both = dot(m_ref[band], high)
    return both[0:PAD] + both[PAD:] + dot(m_ref[band, 0:PAD], low)


def spread_level0(values, w0_ref):
    high, low = split(stack(values))
    w_high, w_low = w0_ref[:, 0:256], w0_ref[:, 256:512]
    out = dot_t(high, w_high) + dot_t(low, w_high) + dot_t(high, w_low)
    return [out[i * PAD : i * PAD + PAD] for i in range(len(values))]


def spread_other(level, values, w_ref, ww_ref):
    high, low = split(stack(values))
    pair = jnp.concatenate([high, low], axis=1)
    out = dot_t(pair, ww_ref[level - 1]) + dot_t(high, w_ref[level - 1, :, 128:256])
    return [out[i * PAD : i * PAD + PAD] for i in range(len(values))]


OWN_BASE = (0, 8, 12, 14)
GOT = {(0, -1): 0, (0, 8): 1, (1, -1): 2, (1, 4): 3, (1, 5): 4, (2, -1): 5, (2, 2): 6, (2, 3): 7, (3, -1): 8, (3, 1): 9}


def pick_at(got_ref, far_ref, at):
    table = {slot(level, index): (got_ref, place) for (level, index), place in GOT.items()}
    table[slot(3, 2)] = (far_ref, 0)

    def pick(place):
        ref, i = table[place]
        return ref[i, at, 0:128], ref[i, at, 128:256]

    return pick


def own_at(own_ref, at):
    def pick(place):
        level = max(i for i in range(LEVELS) if BASE[i] <= place)
        i = OWN_BASE[level] + place - slot(level, 0)
        return own_ref[i, at, 0:128], own_ref[i, at, 128:256]

    return pick


def weights_kernel(taps_ref, filt_ref, w0_ref, w_ref, ww_ref):
    write_filters(taps_ref, filt_ref)
    write_weights(filt_ref, w0_ref, w_ref, ww_ref)


def first_kernel(filt_ref, x_ref, hi_ref, lo_ref):
    flags = edge_flags()

    def chunk(c, carry):
        start = pl.multiple_of(c * (16 * ROWS), 16 * ROWS)
        rows = {r: x_ref[pl.ds(start + r, 16, stride=ROWS), :] for r in range(ROWS)}
        at = pl.ds(pl.multiple_of(c * 16, 16), 16)
        store_split(hi_ref, lo_ref, latitude_analysis(rows, filt_ref, flags), at)
        return carry

    lax.fori_loop(0, 8, chunk, 0)
    top = lax.broadcasted_iota(jnp.int32, (8, LANES), 0) == 0
    rows = {}
    for r in range(ROWS):
        head = x_ref[pl.ds(128 * ROWS + r, 8, stride=ROWS), :]
        tail = jnp.where(top, x_ref[136 * ROWS + r : 136 * ROWS + r + 1, :], 0.0)
        rows[r] = jnp.concatenate([head, tail], axis=0)
    store_split(hi_ref, lo_ref, latitude_analysis(rows, filt_ref, flags), slice(128, 144))


def side_kernel(hi_ref, lo_ref, w0_ref, w_ref, side_ref, far_ref):
    tiles, share = sums_message(hi_ref, lo_ref, w0_ref, w_ref, jnp.logical_not(is_even()), 2)
    put(side_ref, tiles)
    far_ref[...] = pack_coarse(share)


def mate_kernel(hi_ref, lo_ref, w0_ref, w_ref, after_ref, mate_ref):
    del after_ref
    tiles, _ = sums_message(hi_ref, lo_ref, w0_ref, w_ref, is_even(), 0)
    put(mate_ref, tiles)


def own_kernel(hi_ref, lo_ref, w0_ref, w_ref, c0_ref, c1_ref, c1b_ref, c2_ref, c3_ref, c3up_ref):
    level0, others = bands(hi_ref, lo_ref, w0_ref, w_ref)
    c0_ref[0], c0_ref[1] = level0(slot(0, 0), slot(0, 7))
    c1_ref[:, 0:128], c1_ref[:, 128:256], c1b_ref[...] = others(1, slot(1, 0), slot(1, 1), slot(1, 3))
    c2_ref[:, 0:128], c2_ref[:, 128:256] = others(2, slot(2, 0), slot(2, 1))
    c3_ref[...], c3up_ref[...] = others(3, slot(3, 0), slot(3, 1))


def inner_kernel(hi_ref, lo_ref, w0_ref, w_ref, m_ref, after_ref, y0_ref, y1_ref):
    del after_ref
    level0, others = bands(hi_ref, lo_ref, w0_ref, w_ref)
    y1_ref[...] = apply_vertical(m_ref, 1, others(1, slot(1, 2))[0])
    for i, c0 in enumerate(level0(*[slot(0, i) for i in range(1, 7)])):
        y0_ref[i] = apply_vertical(m_ref, 0, c0)


def vertical_kernel(m_ref, filt_ref, c0_ref, c1_ref, c1b_ref, c2_ref, mate_ref, side_ref,
                    y0_ref, y1_ref, y1b_ref, y2_ref, mate_out_ref, side_out_ref):
    below, above = received(mate_ref, side_ref, 4, 4)
    below, above = unpack(below), unpack(above)
    c2 = c2_ref[...]
    y2 = apply_vertical(m_ref, 2, jnp.concatenate([c2[:, 0:128] + below[2], c2[:, 128:256] + below[5] + above[2]], axis=1))
    c1 = c1_ref[...]
    y1 = apply_vertical(m_ref, 1, jnp.concatenate([c1[:, 0:128] + below[1], c1[:, 128:256] + three_bands(below[4], filt_ref)], axis=1))
    y1b = apply_vertical(m_ref, 1, c1b_ref[...] + above[1])
    first = apply_vertical(m_ref, 0, c0_ref[0] + below[0])
    last = apply_vertical(m_ref, 0, c0_ref[1] + above[0])
    y0_ref[0] = first
    y0_ref[1] = last
    y1_ref[...] = y1
    y1b_ref[...] = y1b
    y2_ref[...] = y2
    none = jnp.zeros((PAD, LANES), F32)
    sums = two_sums(y1[:, 128:256], filt_ref)
    down = pack(first, y1[:, 0:128], y2[:, 0:128], none, sums, y2[:, 128:256])
    up = pack(last, y1b, y2[:, 128:256], none, sums, y2[:, 128:256])
    even = is_even()
    put(side_out_ref, [jnp.where(even, d, u) for d, u in zip(down, up)])
    put(mate_out_ref, [jnp.where(even, u, d) for d, u in zip(down, up)])


def coarse_kernel(m_ref, c3_ref, c3up_ref, far_ref, mate_ref, side_ref, passed_ref, mate_in_ref, side_in_ref,
                  y3_ref, mate_out_ref, side_out_ref):
    even = is_even()
    place = lax.axis_index("lat")
    last = lax.axis_size("lat") - 1
    lane = lane_ids(PAD)
    from_side = jnp.where((place == 0) | (place == last), 0.0, pltpu.roll(part(side_ref, 3), 32, 1))
    passed = far_of(part(passed_ref, 3, TAIL))
    passed = jnp.where(even, unpack_coarse(far_ref[...]), jnp.where(place == 1, 0.0, passed))
    mine = c3_ref[...] + pltpu.roll(part(mate_ref, 3), 32, 1) + from_side + passed
    coarse = jnp.where(place == 0, 0.0, far_of(part(side_ref, 3)))
    above = jnp.where(place == last - 1, 0.0, pltpu.roll(part(passed_ref, 3, TAIL), 32, 1))
    other = far_of(part(mate_ref, 3)) + c3up_ref[...] + coarse + above
    both = jnp.concatenate([mine, other], axis=1)
    detail, smooth = apply_vertical(m_ref, 3, both), apply_vertical(m_ref, 4, both)
    y3 = jnp.where(lane < 24, detail[:, 0:128], smooth[:, 0:128])
    y3_ref[...] = y3
    moved = pltpu.roll(y3, 96, 1)
    mate_out_ref[...] = mate_in_ref[...]
    put_one(mate_out_ref, 3, jnp.where(lane < 96, part(mate_in_ref, 3), moved))
    side_out_ref[...] = side_in_ref[...]
    y3_other = jnp.where(lane < 24, detail[:, 128:256], smooth[:, 128:256])
    put_one(side_out_ref, 3, with_far(jnp.where(lane < 96, part(side_in_ref, 3), moved), y3_other))


def spread_kernel(filt_ref, w0_ref, w_ref, ww_ref, y0c_ref, y1c_ref, y0_ref, y1_ref, y1b_ref, y2_ref, y3_ref, sums_ref,
                  own_ref):
    level0 = [y0_ref[i // 7] if i in (0, 7) else y0c_ref[i - 1] for i in range(8)]
    level1 = [y1_ref[:, 0:128], y1_ref[:, 128:256], y1c_ref[...], y1b_ref[...]]
    level2 = [y2_ref[:, 0:128], y2_ref[:, 128:256]]
    wide = spread_level0(level0, w0_ref)
    for level, values in ((1, level1), (2, level2), (3, [y3_ref[...]])):
        wide += spread_other(level, values, w_ref, ww_ref)
    for i, values in enumerate(wide):
        own_ref[i] = values

    def chunk(c, carry):
        at = pl.ds(pl.multiple_of(c * 16, 16), 16)
        for place, total in own_sums(own_at(own_ref, at), filt_ref).items():
            sums_ref[place, at, :] = total
        return carry

    lax.fori_loop(0, 9, chunk, 0)


def received_kernel(w0_ref, w_ref, ww_ref, mate_ref, side_ref, got_ref):
    below, above = received(mate_ref, side_ref, 4, 4)
    below, above = unpack(below), unpack(above)
    wide = spread_level0([below[0], above[0]], w0_ref)
    wide += spread_other(1, [below[1], above[1], bands_of_sums(above[4])], w_ref, ww_ref)
    wide += spread_other(2, [below[2], above[2], above[5]], w_ref, ww_ref)
    wide += spread_other(3, [below[3], above[3]], w_ref, ww_ref)
    for i, values in enumerate(wide):
        got_ref[i] = values


def spread_coarse(side_ref, passed_ref, w_ref, ww_ref, far_ref):
    value = jnp.where(is_even(), pltpu.roll(part(passed_ref, 3, TAIL), 32, 1), far_of(part(side_ref, 3)))
    value = jnp.where(lax.axis_index("lat") >= lax.axis_size("lat") - 2, 0.0, value)
    far_ref[0] = spread_other(3, [value], w_ref, ww_ref)[0]


def middle_kernel(filt_ref, w_ref, ww_ref, sums_ref, got_ref, side_ref, passed_ref, hi_ref, lo_ref, far_ref):
    flags = edge_flags()
    spread_coarse(side_ref, passed_ref, w_ref, ww_ref, far_ref)

    def chunk(c, carry):
        at = pl.ds(pl.multiple_of(c * 16, 16), 16)
        rows = latitude_synthesis(pick_at(got_ref, far_ref, at), lambda i: sums_ref[i, at, :], filt_ref, flags)
        store_split(hi_ref, lo_ref, latitude_analysis(rows, filt_ref, flags), at)
        return carry

    lax.fori_loop(0, 9, chunk, 0)


def last_kernel(filt_ref, w_ref, ww_ref, sums_ref, got_ref, side_ref, passed_ref, out_hbm, far_ref, out_ref, sems):
    flags = edge_flags()
    spread_coarse(side_ref, passed_ref, w_ref, ww_ref, far_ref)

    def leave(c):
        piece = pl.ds(pl.multiple_of(c * (16 * ROWS), 16 * ROWS), 16 * ROWS)
        return pltpu.make_async_copy(out_ref.at[piece, :], out_hbm.at[piece, :], sems.at[c])

    def chunk(c, carry):
        at = pl.ds(pl.multiple_of(c * 16, 16), 16)
        rows = latitude_synthesis(pick_at(got_ref, far_ref, at), lambda i: sums_ref[i, at, :], filt_ref, flags)
        start = pl.multiple_of(c * (16 * ROWS), 16 * ROWS)
        for r, values in rows.items():
            out_ref[pl.ds(start + r, 16, stride=ROWS), :] = values
        leave(c).start()
        return carry

    lax.fori_loop(0, 8, chunk, 0)
    end = slice(128, 144)
    rows = latitude_synthesis(pick_at(got_ref, far_ref, end), lambda i: sums_ref[i, end, :], filt_ref, flags)
    for r, values in rows.items():
        out_ref[pl.ds(128 * ROWS + r, 8, stride=ROWS), :] = values[0:8]
        out_ref[136 * ROWS + r : 136 * ROWS + r + 1, :] = values[8:9]
    rest = pl.ds(128 * ROWS, 9 * ROWS)
    tail = pltpu.make_async_copy(out_ref.at[rest, :], out_hbm.at[rest, :], sems.at[8])
    tail.start()
    for c in range(8):
        leave(c).wait()
    tail.wait()


def prepare_kernel(turned, m_ref, after_ref, out_ref, wide_ref):
    del after_ref
    levels = m_ref.shape[1]
    wide_ref[...] = jnp.zeros_like(wide_ref)
    for band in range(m_ref.shape[0]):
        wide_ref[0:levels, 0:levels] = m_ref[band]
        matrix = wide_ref[...].T if turned else wide_ref[...]
        high, low = split(matrix[0:PAD])
        out_ref[band, 0:PAD, :] = high
        out_ref[band, PAD : 2 * PAD, :] = low


VMEM = pl.BlockSpec(memory_space=pltpu.VMEM)
SMEM = pl.BlockSpec(memory_space=pltpu.SMEM)
HBM = pl.BlockSpec(memory_space=pltpu.HBM)
ANY = pl.BlockSpec(memory_space=pl.ANY)

MESSAGE = ((4 * MAIN + 8, LANES), F32)
FAR = ((40, LANES), F32)
WEIGHTS = (((80, LANES), F32), ((256, 512), BF16), ((3, 256, 256), BF16), ((3, 256, 256), BF16))
HALVES = (((SLOTS, PAD, 256), BF16),) * 2
EDGES = (((2, PAD, 256), F32), ((PAD, 256), F32), ((PAD, LANES), F32), ((PAD, 256), F32))
COARSEST = ((PAD, LANES), F32)
INNER = (((6, PAD, 256), F32), ((PAD, LANES), F32))
OWN_SUMS = ((SUMS, PAD, LANES), F32)
OWN_WIDE = pltpu.VMEM((15, PAD, 256), F32)
GOT_WIDE = ((10, PAD, 256), F32)
FAR_WIDE = pltpu.VMEM((1, PAD, 256), F32)


def call(kernel, in_specs, outs, scratch, limit, out_spec=VMEM):
    return pl.pallas_call(
        kernel,
        out_shape=[jax.ShapeDtypeStruct(shape, dtype) for shape, dtype in outs],
        in_specs=in_specs,
        out_specs=[out_spec] * len(outs),
        scratch_shapes=scratch,
        compiler_params=pltpu.CompilerParams(vmem_limit_bytes=limit * MIB),
        cost_estimate=pl.CostEstimate(flops=10**9, bytes_accessed=8 * MIB, transcendentals=0),
    )


def swap(values, phase):
    count = lax.axis_size("lat")
    partner = {}
    for i in range(phase, count - 1, 2):
        partner[i], partner[i + 1] = i + 1, i
    return lax.ppermute(values, "lat", [(i, partner.get(i, i)) for i in range(count)])


def pass_up(values):
    count = lax.axis_size("lat")
    return lax.ppermute(values, "lat", [(i, i + 2) for i in range(0, count - 2, 2)])


def on_device(increment, filter_taps, band_roots):
    levels, rows, columns = increment.shape
    flat = increment.reshape(levels * rows, columns)
    filt, w0, w, ww = call(weights_kernel, [SMEM], WEIGHTS, [], 12)(filter_taps)
    hi, lo = call(first_kernel, [VMEM] * 2, HALVES, [], 12)(filt, flat)

    def prepare(turned, after):
        kernel = functools.partial(prepare_kernel, turned)
        wide = [pltpu.VMEM((256, 256), F32)]
        (out,) = call(kernel, [VMEM, ANY], (((5, 2 * PAD, 256), BF16),), wide, 12)(band_roots, after)
        return out

    def half(transposed, hi, lo):
        side, far = call(side_kernel, [VMEM] * 4, (MESSAGE, FAR), [], 12)(hi, lo, w0, w)
        (mate,) = call(mate_kernel, [VMEM] * 4 + [ANY], (MESSAGE,), [], 12)(hi, lo, w0, w, side)
        side, mate, far = swap(side, 1), swap(mate, 0), pass_up(far)
        *edges, c3, c3up = call(own_kernel, [VMEM] * 4, EDGES + (COARSEST, COARSEST), [], 12)(hi, lo, w0, w)
        matrix = prepare(transposed, c3up)
        side, matrix = lax.optimization_barrier((side, matrix))
        passed = swap(side[TAIL:], 0)
        *edges, mate_out, side_out = call(
            vertical_kernel, [VMEM] * 8, EDGES + (MESSAGE, MESSAGE), [], 12
        )(matrix, filt, *edges, mate, side)
        y3, mate, side = call(coarse_kernel, [VMEM] * 9, (COARSEST, MESSAGE, MESSAGE), [], 12)(
            matrix, c3, c3up, far, mate, side, passed, mate_out, side_out
        )
        side, mate = swap(side, 1), swap(mate, 0)
        y0c, y1c = call(inner_kernel, [VMEM] * 5 + [ANY], INNER, [], 12)(hi, lo, w0, w, matrix, y3)
        (own,) = call(spread_kernel, [VMEM] * 11, (OWN_SUMS,), [OWN_WIDE], 12)(filt, w0, w, ww, y0c, y1c, *edges, y3)
        side, own = lax.optimization_barrier((side, own))
        passed = swap(side[TAIL:], 0)
        (got,) = call(received_kernel, [VMEM] * 5, (GOT_WIDE,), [], 12)(w0, w, ww, mate, side)
        return filt, w, ww, own, got, side, passed

    ready = half(False, hi, lo)
    hi, lo = call(middle_kernel, [VMEM] * 7, HALVES, [FAR_WIDE], 12)(*ready)
    ready = half(True, hi, lo)
    (out,) = call(
        last_kernel, [VMEM] * 7, (((levels * rows, columns), F32),),
        [FAR_WIDE, pltpu.VMEM((levels * rows, columns), F32), pltpu.SemaphoreType.DMA((9,))], 12, HBM,
    )(*ready)
    return out.reshape(levels, rows, columns)


def solution(mesh):
    placed = (P("member", "lat", None), P(), P())
    return jax.shard_map(
        on_device, mesh=mesh, in_specs=placed, out_specs=P("member", "lat", None), check_vma=False
    )
```
